128 devices in a mesh: seq: 128 (over y, z, x, core).
Axes of the slice: x: 4, y: 4, z: 4, core: 2. Of those that a mesh axis runs over, the one named last changes fastest.
Arguments:
- residual: bfloat16 [16384, 2560], P('seq'), may hold values from -6 to 6
- queries: bfloat16 [16384, 2560], P('seq'), may hold values from -5 to 5, as said below
- keys: bfloat16 [16384, 512], P('seq'), may hold values from -5 to 5
- values: bfloat16 [16384, 512], P('seq'), may hold values from -6 to 6
- out_proj: bfloat16 [2560, 2560], P(None, 'seq'), may hold values from -0.125 to 0.125
- norm_gain: float32 [2560], replicated, may hold values from 0.25 to 1.75
- expert_in: bfloat16 [2560, 2, 106496], P(None, None, 'seq'), may hold values from -0.125 to 0.125
- expert_down: bfloat16 [106496, 2560], P('seq'), may hold values from -0.15625 to 0.15625
- routes: int32 [16384, 2], P('seq'), may hold values from 0 to 63, all different within a row
- gate_ints: int32 [16384, 2], P('seq'), may hold values from 1 to 1023
- modality: int32 [16384], P('seq'), may hold values 0 or 1
- capacity: int32 [64, 2], replicated, may hold values from 1 to 2, as said below
Outputs:
- attended: bfloat16 [16384, 2560], P('seq')
- expert_mix: bfloat16 [16384, 2560], P('seq')
The draws below stay inside these ranges and needn't reach their ends.
Inputs may be any that keep to these rules, and one draw needn't show every extreme that they name: `queries` and `keys`: every element lies between -5 and 5. `routes`: each token names two different experts. `capacity`: some entry equals 2.
All inputs are finite; a program needn't handle non-finite values. No bound on the sum of `modality` on one device may be relied on, other than what follows from the above.
Results may differ from the reference program's by a relative error of at most 0.0086.
Values may be sent and summed in bfloat16 or wider, within the bound.
A program may use at most 192 MiB of HBM per device.

```python
import math
import jax
import jax.numpy as jnp
from jax import lax

D = 2560
HEADS = 20
KV_HEADS = 4
HEAD = 128
WINDOW = 1024
EXPERTS = 64
FF = 1664
TOK_DEV = 128
CAP = 2
TOKENS = 16384
N_SEQ = 128


def draw_queries(key, part):
    drawn = jnp.clip(jax.random.normal(jax.random.fold_in(key, 3), (TOKENS, HEADS * HEAD), jnp.float32), -5.0, 5.0)
    return drawn.astype(jnp.bfloat16)


def draw_keys(key, part):
    drawn = jnp.clip(jax.random.normal(jax.random.fold_in(key, 4), (TOKENS, KV_HEADS * HEAD), jnp.float32), -5.0, 5.0)
    return drawn.astype(jnp.bfloat16)


def draw_capacity(key, part):
    cap_table = jax.random.randint(jax.random.fold_in(key, 21), (EXPERTS * 2,), 1, CAP + 1)
    full_spot = jax.random.randint(jax.random.fold_in(key, 22), (), 0, EXPERTS * 2)
    cap_table = jnp.where(jnp.arange(EXPERTS * 2) == full_spot, CAP, cap_table)
    return cap_table.reshape(EXPERTS, 2).astype(jnp.int32)


def set_ends(values, own_key, least, largest):
    longest = values.shape.index(max(values.shape))
    spots = []
    for shift in (0, 1):
        where = [jax.random.randint(jax.random.fold_in(own_key, axis), (), 0, length) for axis, length in enumerate(values.shape)]
        where[longest] = (where[longest] + shift) % values.shape[longest]
        spots.append(tuple(where))
    return values.at[spots[0]].set(least).at[spots[1]].set(largest)


def steps_of(own_key, dims, split, smallest, high):
    level = 1.0
    for axis_at, parts in split:
        heights = jax.random.uniform(jax.random.fold_in(jax.random.fold_in(own_key, 6), axis_at), (parts,), jnp.float32, smallest / len(split), high / len(split))
        level = level * jnp.repeat(jnp.exp(heights), dims[axis_at] // parts).reshape((-1,) + (1,) * (len(dims) - 1 - axis_at))
    return level


def picks_of(stream_key, rows, amount, top, lift):
    ranking = jax.random.permutation(jax.random.fold_in(stream_key, 1), amount)
    pull = ranking
    for power in range(3):
        pull = pull * pull // amount
    pull = pull * lift // amount
    lots = jax.random.randint(jax.random.fold_in(stream_key, 2), (rows, amount), 0, 4096) + pull
    fixed_rows = jax.random.permutation(jax.random.fold_in(stream_key, 3), rows)[jnp.arange(amount) % rows]
    lots = jnp.where(jnp.arange(rows)[:, None] == fixed_rows[None, :], 1 << 14, lots)
    score = lots * amount + jnp.arange(amount)
    return lax.top_k(score.astype(jnp.int32), top)[1].astype(jnp.int32)


def bell_draw(own_key, shape, deviation, bound, cuts=(), held_as=jnp.bfloat16):
    result = deviation * jax.random.normal(own_key, shape, jnp.float32)
    if cuts:
        result = result * steps_of(own_key, shape, cuts, -0.22, 0.18)
    return jnp.clip(result, -bound, bound).astype(held_as)


def setup_inputs(seed: int = 0) -> dict:
    key_list = jax.random.split(jax.random.key(seed), 13)
    return {
        "residual": bell_draw(key_list[0], (TOKENS, D), 1.0, 6.0, ((0, 128),)),
        "queries": draw_queries(jax.random.fold_in(key_list[12], 71), 0),
        "keys": draw_keys(jax.random.fold_in(key_list[12], 71), 0),
        "values": bell_draw(key_list[3], (TOKENS, KV_HEADS * HEAD), 1.0, 6.0, ((0, 128),)),
        "out_proj": bell_draw(key_list[4], (HEADS * HEAD, D), (HEADS * HEAD) ** -0.5, 0.125, ((1, 128),)),
        "norm_gain": jnp.clip(1.0 + 0.15 * jax.random.normal(key_list[5], (D,), jnp.float32), 0.25, 1.75),
        "expert_in": bell_draw(key_list[6], (D, 2, EXPERTS * FF), D ** -0.5, 0.125, ((2, 128),)),
        "expert_down": bell_draw(key_list[7], (EXPERTS * FF, D), FF ** -0.5, 0.15625, ((0, 128),)),
        "routes": picks_of(key_list[8], TOKENS, EXPERTS, 2, 512),
        "gate_ints": set_ends(jax.random.randint(key_list[9], (TOKENS, 2), 1, 1024), jax.random.fold_in(key_list[9], 1), 1, 1023).astype(jnp.int32),
        "modality": set_ends((jax.random.randint(key_list[10], (TOKENS,), 0, 2) < 1).astype(jnp.int32), jax.random.fold_in(key_list[10], 1), 0, 1),
        "capacity": draw_capacity(jax.random.fold_in(key_list[12], 71), 0),
    }


def attend(queries, keys, values):
    row_total = queries.shape[0]
    q_group = HEADS // KV_HEADS
    q_block = math.gcd(row_total, 512)
    q_blocks = queries.reshape(row_total // q_block, q_block, KV_HEADS, q_group, HEAD)
    keys_padded = jnp.pad(keys, ((WINDOW, 0), (0, 0))).reshape(row_total + WINDOW, KV_HEADS, HEAD)
    values_padded = jnp.pad(values, ((WINDOW, 0), (0, 0))).reshape(row_total + WINDOW, KV_HEADS, HEAD)

    def one_block(block_idx):
        first_row = (block_idx * q_block).astype(jnp.int32)
        q_here = lax.dynamic_index_in_dim(q_blocks, block_idx, 0, keepdims=False).astype(jnp.float32)
        k_here = lax.dynamic_slice_in_dim(keys_padded, first_row, q_block + WINDOW, 0).astype(jnp.float32)
        v_here = lax.dynamic_slice_in_dim(values_padded, first_row, q_block + WINDOW, 0).astype(jnp.float32)
        scores = jnp.einsum('qhgd,khd->hgqk', q_here, k_here) * HEAD ** (-0.5)
        q_pos = first_row + jnp.arange(q_block, dtype=jnp.int32)
        k_pos = first_row - WINDOW + jnp.arange(q_block + WINDOW, dtype=jnp.int32)
        visible = (k_pos[None, :] <= q_pos[:, None]) & (k_pos[None, :] > q_pos[:, None] - WINDOW) & (k_pos[None, :] >= 0)
        scores = jnp.where(visible, scores, -jnp.inf)
        row_max = lax.optimization_barrier(jnp.max(scores, -1, keepdims=True))
        weights_raw = jnp.exp(scores - row_max)
        probs_bf = (weights_raw / lax.optimization_barrier(jnp.sum(weights_raw, -1, keepdims=True))).astype(jnp.bfloat16)
        context = jnp.einsum('hgqk,khd->qhgd', probs_bf.astype(jnp.float32), v_here)
        return context.reshape(q_block, HEADS * HEAD).astype(jnp.bfloat16)
    mapped = lax.map(one_block, jnp.arange(row_total // q_block, dtype=jnp.int32))
    return mapped.reshape(row_total, HEADS * HEAD)

def experts_ref(normed, expert_in, expert_down, routes, gate_ints, modality, capacity):
    split_ways = max(1, N_SEQ // EXPERTS)
    slot_count = 2 * CAP
    expert = routes.reshape(N_SEQ, TOK_DEV * 2)
    mode_flag = jnp.repeat(modality, 2).reshape(N_SEQ, TOK_DEV * 2)
    slot_key = expert * 2 + mode_flag
    onehot = (slot_key[:, :, None] == jnp.arange(2 * EXPERTS, dtype=jnp.int32)[None, None, :]).astype(jnp.int32)
    before = jnp.cumsum(onehot, axis=1) - onehot
    rank_in = lax.optimization_barrier(jnp.sum(before * onehot, -1))
    limit_of = capacity.reshape(-1)[slot_key]
    kept_mask = rank_in < limit_of
    source = jnp.arange(N_SEQ, dtype=jnp.int32)[:, None]
    place_at = expert * (N_SEQ * slot_count) + source * slot_count + mode_flag * CAP + rank_in
    outside = EXPERTS * N_SEQ * slot_count
    place_at = jnp.where(kept_mask, place_at, outside).astype(jnp.int32)
    token_ids = jnp.repeat(jnp.arange(TOKENS, dtype=jnp.int32), 2)
    slot_table = jnp.full((outside,), TOKENS, jnp.int32).at[place_at.reshape(-1)].set(token_ids, mode='drop')
    slot_table = slot_table.reshape(EXPERTS, N_SEQ * slot_count)
    padded = jnp.concatenate([normed, jnp.zeros((1, D), jnp.bfloat16)], 0)
    part_width = FF // split_ways

    def one_expert(expert_id):
        picked_rows = padded[slot_table[expert_id]]
        zero_at = jnp.zeros((), jnp.int32)
        first_col = (expert_id * FF).astype(jnp.int32)
        weights_here = lax.dynamic_slice(expert_in, (zero_at, zero_at, first_col), (D, 2, FF))
        gate_val = jnp.dot(picked_rows, weights_here[:, 0, :], preferred_element_type=jnp.float32)
        up_val = jnp.dot(picked_rows, weights_here[:, 1, :], preferred_element_type=jnp.float32)
        active = (jax.nn.silu(gate_val) * up_val).astype(jnp.bfloat16)
        down_rows = lax.dynamic_slice_in_dim(expert_down, first_col, FF, 0)
        summed = jnp.zeros((N_SEQ * slot_count, D), jnp.float32)
        for piece_idx in range(split_ways):
            lo_col = piece_idx * part_width
            partial_value = jnp.dot(active[:, lo_col:lo_col + part_width], down_rows[lo_col:lo_col + part_width], preferred_element_type=jnp.float32).astype(jnp.bfloat16)
            partial_value = lax.optimization_barrier(partial_value)
            summed = summed + partial_value.astype(jnp.float32)
        return summed.astype(jnp.bfloat16)
    expert_rows = lax.map(one_expert, jnp.arange(EXPERTS, dtype=jnp.int32))
    flat_rows = expert_rows.reshape(-1, D)
    pick_at = jnp.where(kept_mask, place_at, 0).reshape(-1).astype(jnp.int32)
    chosen_rows = flat_rows[pick_at].astype(jnp.float32).reshape(TOKENS, 2, D)
    gate_scale = jnp.where(kept_mask.reshape(TOKENS, 2), gate_ints.astype(jnp.float32) / 1024.0, 0.0)
    return lax.optimization_barrier(jnp.sum(gate_scale[:, :, None] * chosen_rows, 1)).astype(jnp.bfloat16)

def reference(residual, queries, keys, values, out_proj, norm_gain, expert_in, expert_down, routes, gate_ints, modality, capacity):
    context = attend(queries, keys, values)
    attended = jnp.dot(context, out_proj, preferred_element_type=jnp.float32).astype(jnp.bfloat16)
    attended = lax.optimization_barrier(attended)
    hidden = residual.astype(jnp.float32) + attended.astype(jnp.float32)
    normed = (hidden * lax.rsqrt(lax.optimization_barrier(jnp.mean(hidden * hidden, -1, keepdims=True)) + 1e-05) * norm_gain).astype(jnp.bfloat16)
    expert_mix = experts_ref(normed, expert_in, expert_down, routes, gate_ints, modality, capacity)
    return (attended, expert_mix)
```

```python
import functools

import jax
import jax.numpy as jnp
from jax import lax
from jax.experimental import pallas as pl
from jax.experimental.pallas import tpu as pltpu
from jax.sharding import PartitionSpec as P

HEADS = 20
KV_HEADS = 4
HEAD = 128
GROUP = HEADS // KV_HEADS
WINDOW = 1024
EXPERTS = 64
CAP = 2
D = 2560
TOK = 128
NDEV = 128
MESH = pl.DeviceIdType.MESH
DMA = pltpu.SemaphoreType.DMA
DELTAS = (1, 3, 2)
PARTS = (((2, 1, 0), 0, 7), ((1, 0, 2), 7, 5), ((0, 2, 1), 12, 8))
KT = D // 128


def coords(me):
    return [me // 32, (me // 8) % 4, (me // 2) % 4, me % 2]


def dev(cs):
    return ((cs[0] * 4 + cs[1]) * 4 + cs[2]) * 2 + cs[3]


def shift(cs, dim, d):
    cs = list(cs)
    cs[dim] = lax.rem(cs[dim] + d, 4)
    return cs


def wslice(cs, alld, fixed, t0, tn):
    idx = [slice(None) if d in alld else cs[d] for d in range(3)]
    for d, v in fixed.items():
        idx[d] = v
    return tuple(idx) + (pl.ds(t0, tn),)


def attend_kernel(
    wa, wb, q, k, v, res, gain, att_out, norm_out,
    G, B1, BX, Kb, Vb, bias, ctx, attp, attt,
    s1, r1, s2, r2, s3, r3, s4, r4, sb1, rb1, sb2, rb2, sb3, rb3, sb4, rb4,
    kvs, kvr, cxs, cxr, ats, atr, lsem,
):
    me = lax.axis_index("seq")
    cs = coords(me)
    y, z, x, core = cs
    bar = pltpu.get_barrier_semaphore()
    sib = dev([y, z, x, 1 - core])
    peers = [dev(shift(cs, dim, d)) for dim in range(3) for d in DELTAS]
    peers += [sib, lax.rem(me + 8, NDEV), lax.rem(me + NDEV - 8, NDEV)]
    for p in peers:
        pl.semaphore_signal(bar, inc=1, device_id=(p,), device_id_type=MESH)
    own = [
        pltpu.make_async_copy(wa, G.at[y, z, x], lsem.at[0]),
        pltpu.make_async_copy(wb, B1.at[x], lsem.at[1]),
        pltpu.make_async_copy(k, Kb.at[8], lsem.at[2]),
        pltpu.make_async_copy(v, Vb.at[8], lsem.at[3]),
    ]
    for c in own:
        c.start()
    row = lax.broadcasted_iota(jnp.int32, (TOK, TOK), 0)
    col = lax.broadcasted_iota(jnp.int32, (TOK, TOK), 1)
    for j in range(9):
        ok = me - 8 + j >= 0
        if j == 0:
            m = (col > row) & ok
        elif j == 8:
            m = col <= row
        else:
            m = (col >= 0) & ok
        bias[:, j * TOK:(j + 1) * TOK] = jnp.where(m, 0.0, -jnp.inf)
    for c in own:
        c.wait()
    pl.semaphore_wait(bar, len(peers))
    sends = []

    def rc(src, dst, ss, rs, dv):
        c = pltpu.make_async_remote_copy(
            src_ref=src, dst_ref=dst, send_sem=ss, recv_sem=rs, device_id=(dv,), device_id_type=MESH
        )
        c.start()
        sends.append(c)
        return c

    nxt = lax.rem(me + 8, NDEV)
    kv4 = [rc(b_.at[8], b_.at[0], kvs.at[n, 3], kvr.at[n, 3], nxt) for n, b_ in enumerate((Kb, Vb))]
    kvx = []
    for dlt in (1, 2, 3):
        tgt = dev(shift(cs, 2, dlt))
        pair = []
        for n, b_ in enumerate((Kb, Vb)):
            pair.append(
                tuple(
                    pltpu.make_async_remote_copy(
                        src_ref=b_.at[s], dst_ref=b_.at[8 - 2 * dlt], send_sem=kvs.at[n, dlt - 1],
                        recv_sem=kvr.at[n, dlt - 1], device_id=(tgt,), device_id_type=MESH,
                    )
                    for s in (8, 0)
                )
            )
        kvx.append(pair)
        sends += [p_[0] for p_ in pair]

        @pl.when(x + dlt < 4)
        def _():
            for p_ in pair:
                p_[0].start()

    p1 = []
    for pi, ((a, bb, c), t0, tn) in enumerate(PARTS):
        sl = wslice(cs, (), {}, t0, tn)
        p1.append(
            [rc(G.at[sl], G.at[sl], s1.at[pi, i], r1.at[pi, i], dev(shift(cs, a, d))) for i, d in enumerate(DELTAS)]
        )
    pb1 = [rc(B1.at[x], B1.at[x], sb1.at[i], rb1.at[i], dev(shift(cs, 2, d))) for i, d in enumerate(DELTAS)]

    p3 = [[None] * 4 for _ in PARTS]
    pb3 = [None] * 4

    def chunk_send(pi, i, bi):
        (a, bb, c), t0, tn = PARTS[pi]
        sl = wslice(cs, (a,), {bb: bi}, t0, tn)
        p3[pi][i] = [
            rc(G.at[sl], G.at[sl], s3.at[pi, i, n], r3.at[pi, i, n], dev(shift(cs, c, d)))
            for n, d in enumerate(DELTAS[:2])
        ]
        if pi == 0:
            pb3[i] = [
                rc(BX.at[y, bi], BX.at[y, bi], sb3.at[i, n], rb3.at[i, n], dev(shift(cs, 0, d)))
                for n, d in enumerate(DELTAS[:2])
            ]

    p2 = []
    pb2 = []
    for pi, ((a, bb, c), t0, tn) in enumerate(PARTS):
        for n in range(3):
            p1[pi][n].wait_recv()
        if pi == 0:
            for n in range(3):
                pb1[n].wait_recv()
            src = [[B1[xx, i].astype(jnp.float32) for i in range(5)] for xx in range(4)]
            for kq in range(4):
                for i in range(5):
                    BX[y, z, kq * 5 + i] = jnp.concatenate(
                        [src[xx][i][kq * 4:kq * 4 + 4] for xx in range(4)], 0
                    ).astype(jnp.bfloat16)
        sl = wslice(cs, (a,), {}, t0, tn)
        p2.append(
            [rc(G.at[sl], G.at[sl], s2.at[pi, i], r2.at[pi, i], dev(shift(cs, bb, d))) for i, d in enumerate(DELTAS)]
        )
        if pi == 0:
            pb2 = [
                rc(BX.at[y, z], BX.at[y, z], sb2.at[i], rb2.at[i], dev(shift(cs, 1, d)))
                for i, d in enumerate(DELTAS)
            ]
        chunk_send(pi, 0, cs[bb])

    for c in kv4:
        c.wait_recv()
    for dlt in (1, 2, 3):

        @pl.when(x + dlt >= 4)
        def _():
            for p_ in kvx[dlt - 1]:
                p_[1].start()

    for i, d in enumerate(DELTAS):
        for pi, ((a, bb, c), t0, tn) in enumerate(PARTS):
            p2[pi][i].wait_recv()
            if pi == 0:
                pb2[i].wait_recv()
            chunk_send(pi, i + 1, lax.rem(cs[bb] + 4 - d, 4))

    rl = []

    def relay(i):
        for pi, ((a, bb, c), t0, tn) in enumerate(PARTS):
            bi = cs[bb] if i == 0 else lax.rem(cs[bb] + 4 - DELTAS[i - 1], 4)
            h = tn // 2
            for n, (dfrom, dto, lo, cnt) in enumerate(((3, 1, 0, h), (1, 3, h, tn - h))):
                p3[pi][i][n].wait_recv()
                s_ = wslice(cs, (a,), {bb: bi, c: lax.rem(cs[c] + dfrom, 4)}, t0 + lo, cnt)
                rl.append(rc(G.at[s_], G.at[s_], s4.at[pi, i, n], r4.at[pi, i, n], dev(shift(cs, c, dto))))
                if pi == 0:
                    pb3[i][n].wait_recv()
                    b_ = BX.at[lax.rem(y + dfrom, 4), bi, pl.ds(10 * n, 10)]
                    rl.append(rc(b_, b_, sb4.at[i, n], rb4.at[i, n], dev(shift(cs, 0, dto))))

    relay(0)
    kvd = []
    for p_ in kvx:
        for n in range(2):
            p_[n][0].wait_recv()
    for i in range(4):
        src = 8 - 2 * i - 2 * core
        for n, b_ in enumerate((Kb, Vb)):
            kvd.append(rc(b_.at[src], b_.at[7 - 2 * i], kvs.at[n, 4 + i], kvr.at[n, 4 + i], sib))
    relay(1)
    for c in kvd:
        c.wait_recv()

    scale = HEAD ** (-0.5)
    cxc = []
    for h in range(KV_HEADS):
        hs = slice(h * HEAD, (h + 1) * HEAD)
        kh = Kb[:, :, hs].reshape(9 * TOK, HEAD)
        vh = Vb[:, :, hs].reshape(9 * TOK, HEAD)
        for g in range(GROUP):
            qs = slice((h * GROUP + g) * HEAD, (h * GROUP + g + 1) * HEAD)
            s = lax.dot_general(
                q[:, qs], kh, (((1,), (1,)), ((), ())), preferred_element_type=jnp.float32
            ) * scale + bias[...]
            mx = jnp.max(s, -1, keepdims=True)
            e = jnp.exp(s - mx)
            tot = jnp.sum(e, -1, keepdims=True)
            o = jnp.dot(e.astype(jnp.bfloat16), vh, preferred_element_type=jnp.float32)
            ctx[core, h, :, g * HEAD:(g + 1) * HEAD] = (o / tot).astype(jnp.bfloat16)
        cxc.append(rc(ctx.at[core, h], ctx.at[core, h], cxs.at[h], cxr.at[h], sib))
        if h < 2:
            relay(h + 2)
    for c in cxc:
        c.wait_recv()
    for c in rl:
        c.wait_recv()

    def project(tile_pair):
        acc = None
        for kp in range(KT // 2):
            lhs = tile_pair(2 * kp)
            h, off = (2 * kp) // GROUP, (2 * kp) % GROUP
            cols = []
            for t in (2 * kp, 2 * kp + 1):
                hh, oo = t // GROUP, t % GROUP
                cols.append(ctx[:, hh, :, oo * HEAD:(oo + 1) * HEAD].reshape(2 * TOK, HEAD))
            rhs = jnp.concatenate(cols, 1)
            part = lax.dot_general(lhs, rhs, (((1,), (1,)), ((), ())), preferred_element_type=jnp.float32)
            acc = part if acc is None else acc + part
        return acc.astype(jnp.bfloat16)

    def put(first, rows, val):
        attp[core, 0, pl.ds(first, rows)] = val[:, :TOK]
        attp[core, 1, pl.ds(first, rows)] = val[:, TOK:]

    def a_rows(yy, carry):
        def pair(t):
            return jnp.concatenate(
                [G[yy, :, :, t + i].reshape(256, 128) for i in range(2)], 1
            )
        put(yy * 256, 256, project(pair))
        return carry

    lax.fori_loop(0, 4, a_rows, 0)
    put(1024, 256, project(
        lambda t: jnp.concatenate([BX[:, :, t + i].reshape(256, 128) for i in range(2)], 1)
    ))
    xc = rc(attp.at[core, 1 - core], attp.at[core, 1 - core], ats, atr, sib)
    xc.wait_recv()
    mine = [attp.at[0, core], attp.at[1, core]]
    for chip in range(64):
        for c in range(2):
            d0 = 20 * (chip * 2 + c)
            attt[d0:d0 + 16] = mine[c][chip * 16:chip * 16 + 16].astype(jnp.float32)
    for yz in range(16):
        for c in range(2):
            blk = mine[c][1024 + yz * 16:1024 + yz * 16 + 16].astype(jnp.float32)
            for xx in range(4):
                d0 = 20 * ((yz * 4 + xx) * 2 + c) + 16
                attt[d0:d0 + 4] = blk[xx * 4:xx * 4 + 4]
    ssq = jnp.zeros((TOK, 1), jnp.float32)
    for t in range(KT):
        ls = slice(t * 128, (t + 1) * 128)
        a_ = jnp.transpose(attt[ls])
        att_out[:, ls] = a_.astype(jnp.bfloat16)
        hd = res[:, ls].astype(jnp.float32) + a_
        ssq = ssq + jnp.sum(hd * hd, -1, keepdims=True)
    inv = lax.rsqrt(ssq / D + 1e-05)
    for t in range(KT):
        ls = slice(t * 128, (t + 1) * 128)
        hd = res[:, ls].astype(jnp.float32) + att_out[:, ls].astype(jnp.float32)
        norm_out[:, ls] = (hd * inv * gain[:, ls]).astype(jnp.bfloat16)
    for c in sends:
        c.wait_send()


def attend(residual, queries, keys, values, out_proj, norm_gain):
    wt = out_proj.T
    wa = wt[:16].reshape(16, KT, 128).transpose(1, 0, 2)
    wb = wt[16:].reshape(4, 4, 5, 128).transpose(2, 1, 0, 3).reshape(5, 16, 128)
    any_ = pl.BlockSpec(memory_space=pl.ANY)
    vm = pl.BlockSpec(memory_space=pltpu.VMEM)
    bf = jnp.bfloat16
    return pl.pallas_call(
        attend_kernel,
        out_shape=(jax.ShapeDtypeStruct((TOK, D), bf), jax.ShapeDtypeStruct((TOK, D), bf)),
        in_specs=[any_, any_, vm, any_, any_, vm, vm],
        out_specs=(vm, vm),
        scratch_shapes=[
            pltpu.VMEM((4, 4, 4, KT, 16, 128), bf),
            pltpu.VMEM((4, 5, 16, 128), bf),
            pltpu.VMEM((4, 4, KT, 16, 128), bf),
            pltpu.VMEM((9, TOK, KV_HEADS * HEAD), bf),
            pltpu.VMEM((9, TOK, KV_HEADS * HEAD), bf),
            pltpu.VMEM((TOK, 9 * TOK), jnp.float32),
            pltpu.VMEM((2, KV_HEADS, TOK, GROUP * HEAD), bf),
            pltpu.VMEM((2, 2, 1280, TOK), bf),
            pltpu.VMEM((D, TOK), jnp.float32),
            DMA((3, 3)), DMA((3, 3)), DMA((3, 3)), DMA((3, 3)),
            DMA((3, 4, 2)), DMA((3, 4, 2)), DMA((3, 4, 2)), DMA((3, 4, 2)),
            DMA((3,)), DMA((3,)), DMA((3,)), DMA((3,)),
            DMA((4, 2)), DMA((4, 2)), DMA((4, 2)), DMA((4, 2)),
            DMA((2, 8)), DMA((2, 8)), DMA((4,)), DMA((4,)), DMA, DMA, DMA((4,)),
        ],
        compiler_params=pltpu.CompilerParams(
            has_side_effects=True, collective_id=0, vmem_limit_bytes=48 * 2**20
        ),
    )(wa, wb, queries, keys, values, residual, norm_gain.reshape(1, D))


def exchange_kernel(x, o, ssem, rsem, lsem):
    me = lax.axis_index("seq")
    bar = pltpu.get_barrier_semaphore()

    def signal(s, c):
        pl.semaphore_signal(bar, inc=1, device_id=(lax.rem(me + s, NDEV),), device_id_type=MESH)
        return c

    lax.fori_loop(1, NDEV, signal, 0)
    pl.semaphore_wait(bar, NDEV - 1)
    own = pltpu.make_async_copy(x.at[me], o.at[me], lsem)
    own.start()
    cs = coords(me)

    def send(i, c):
        s = (i * 37) % NDEV
        t = dev([(cs[0] + s // 32) % 4, (cs[1] + (s // 8) % 4) % 4, (cs[2] + (s // 2) % 4) % 4, (cs[3] + s % 2) % 2])
        pltpu.make_async_remote_copy(
            src_ref=x.at[t], dst_ref=o.at[me], send_sem=ssem, recv_sem=rsem, device_id=(t,), device_id_type=MESH
        ).start()
        return c

    lax.fori_loop(1, NDEV, send, 0)
    own.wait()
    whole = pl.ds(0, NDEV - 1)
    done = pltpu.make_async_remote_copy(
        src_ref=x.at[whole], dst_ref=o.at[whole], send_sem=ssem, recv_sem=rsem,
        device_id=(lax.rem(me + 1, NDEV),), device_id_type=MESH,
    )
    done.wait_send()
    done.wait_recv()


def exchange(rows, cid):
    return pl.pallas_call(
        exchange_kernel,
        out_shape=jax.ShapeDtypeStruct(rows.shape, rows.dtype),
        in_specs=[pl.BlockSpec(memory_space=pl.ANY)],
        out_specs=pl.BlockSpec(memory_space=pl.ANY),
        scratch_shapes=[DMA, DMA, DMA],
        compiler_params=pltpu.CompilerParams(has_side_effects=True, collective_id=cid),
    )(rows)


def swapped(value):
    return lax.ppermute(value, "seq", [(s, s ^ 1) for s in range(NDEV)])


def body(
    residual, queries, keys, values, out_proj, norm_gain, expert_in, expert_down,
    routes, gate_ints, modality, capacity,
):
    device_pos = lax.axis_index("seq")
    attended, normed = attend(residual, queries, keys, values, out_proj, norm_gain)
    slot_count = 2 * CAP
    chosen = routes.reshape(-1)
    modal_flag = jnp.repeat(modality, 2)
    slot_key = chosen * 2 + modal_flag
    onehot = (slot_key[:, None] == jnp.arange(2 * EXPERTS, dtype=jnp.int32)[None, :]).astype(jnp.int32)
    rank_in = jnp.sum((jnp.cumsum(onehot, 0) - onehot) * onehot, 1)
    limit_of = jnp.sum(onehot * capacity.reshape(1, -1), 1)
    kept_mask = rank_in < limit_of
    column = chosen * slot_count + modal_flag * CAP + rank_in
    select = (
        (column[:, None] == jnp.arange(EXPERTS * slot_count, dtype=jnp.int32)[None, :]) & kept_mask[:, None]
    ).astype(jnp.bfloat16)
    doubled = jnp.repeat(normed, 2, axis=0)
    slot_table = lax.dot_general(
        select, doubled, (((0,), (0,)), ((), ())), preferred_element_type=jnp.float32
    ).astype(jnp.bfloat16)
    hidden_each = expert_in.shape[2]
    own_rows = exchange(slot_table.reshape(NDEV, CAP, D), 1)
    partner = swapped(own_rows)
    is_lower = device_pos % 2 == 0
    first_half = jnp.where(is_lower, own_rows, partner)
    second_half = jnp.where(is_lower, partner, own_rows)
    rows_in = jnp.stack([first_half, second_half], 1).reshape(NDEV, slot_count, D)
    gate_up = jnp.einsum("nkd,dgf->gnkf", rows_in, expert_in, preferred_element_type=jnp.float32)
    active = (jax.nn.silu(gate_up[0]) * gate_up[1]).astype(jnp.bfloat16)
    partial_value = jnp.einsum("nkf,fd->nkd", active, expert_down, preferred_element_type=jnp.float32)
    partial_value = lax.optimization_barrier(partial_value.astype(jnp.bfloat16)).reshape(NDEV, 2, CAP, D)
    keep_own = jnp.where(is_lower, partial_value[:, 0], partial_value[:, 1])
    give_back = jnp.where(is_lower, partial_value[:, 1], partial_value[:, 0])
    taken = swapped(give_back)
    summed = (keep_own.astype(jnp.float32) + taken.astype(jnp.float32)).astype(jnp.bfloat16)
    returned = exchange(summed, 2)
    mixed = returned.reshape(EXPERTS * slot_count, D)
    gathered_rows = jnp.dot(select, mixed, preferred_element_type=jnp.float32).reshape(TOK, 2, D)
    gate_scale = jnp.where(
        kept_mask, gate_ints.reshape(-1).astype(jnp.float32) / 1024.0, 0.0
    ).reshape(TOK, 2, 1)
    expert_mix = jnp.sum(gate_scale * gathered_rows, 1).astype(jnp.bfloat16)
    return (attended, expert_mix)


def solution(mesh):
    placed = (
        P("seq", None), P("seq", None), P("seq", None), P("seq", None), P(None, "seq"), P(),
        P(None, None, "seq"), P("seq", None), P("seq", None), P("seq", None), P("seq"), P(),
    )
    return jax.shard_map(
        body, mesh=mesh, in_specs=placed, out_specs=(P("seq", None), P("seq", None)), check_vma=False
    )
```

```python
import functools

import jax
import jax.numpy as jnp
from jax import lax
from jax.experimental import pallas as pl
from jax.experimental.pallas import tpu as pltpu
from jax.sharding import PartitionSpec as P

HEADS = 20
KV_HEADS = 4
HEAD = 128
GROUP = HEADS // KV_HEADS
WINDOW = 1024
EXPERTS = 64
CAP = 2
D = 2560
TOK = 128
NDEV = 128
MESH = pl.DeviceIdType.MESH
DMA = pltpu.SemaphoreType.DMA
DELTAS = (1, 3, 2)
PARTS = (((2, 1, 0), 0, 7), ((1, 0, 2), 7, 5), ((0, 2, 1), 12, 8))
KT = D // 128


def coords(me):
    return [me // 32, (me // 8) % 4, (me // 2) % 4, me % 2]


def dev(cs):
    return ((cs[0] * 4 + cs[1]) * 4 + cs[2]) * 2 + cs[3]


def shift(cs, dim, d):
    cs = list(cs)
    cs[dim] = lax.rem(cs[dim] + d, 4)
    return cs


def wslice(cs, alld, fixed, t0, tn):
    idx = [slice(None) if d in alld else cs[d] for d in range(3)]
    for d, v in fixed.items():
        idx[d] = v
    return tuple(idx) + (pl.ds(t0, tn),)


def order(i):
    s = (i * 37) % NDEV
    return [s // 32, (s // 8) % 4, (s // 2) % 4, s % 2]


def routing(routes, gates, modal, cap, st, wt):
    rows = 2 * NDEV
    rho = lax.broadcasted_iota(jnp.int32, (rows, TOK), 0)
    key, turn = jnp.right_shift(rho, 1), jnp.bitwise_and(rho, 1)
    mod = modal[...][None, :]
    is0 = key == routes[0:1] * 2 + mod
    is1 = key == routes[1:2] * 2 + mod
    hit = jnp.where(is0 | is1, 1.0, 0.0)
    before = lax.broadcasted_iota(jnp.int32, (TOK, TOK), 0) < lax.broadcasted_iota(jnp.int32, (TOK, TOK), 1)
    rank = jnp.dot(
        hit.astype(jnp.bfloat16), jnp.where(before, 1.0, 0.0).astype(jnp.bfloat16),
        preferred_element_type=jnp.float32,
    )
    rho_e = lax.broadcasted_iota(jnp.int32, (rows, EXPERTS), 0)
    at_e = lax.broadcasted_iota(jnp.int32, (rows, EXPERTS), 1) == jnp.right_shift(rho_e, 2)
    cap_e = jnp.where(jnp.bitwise_and(rho_e, 2) == 0, cap[0:1], cap[1:2]).astype(jnp.float32)
    limit = jnp.sum(jnp.where(at_e, cap_e, 0.0), -1, keepdims=True)
    turn_f = turn.astype(jnp.float32)
    kept = jnp.where((rank == turn_f) & (turn_f < limit), hit, 0.0)
    st[...] = kept.astype(jnp.bfloat16)
    g = jnp.where(is0, gates[0:1], gates[1:2])
    high = jnp.bitwise_and(g, 1016)
    wt[0] = jnp.transpose(high.astype(jnp.float32) * kept).astype(jnp.bfloat16)
    wt[1] = jnp.transpose((g - high).astype(jnp.float32) * kept).astype(jnp.bfloat16)


def layer_kernel(
    w, q, k, v, res, gain, w_in, w_down, routes, gates, modal, cap, att_out, mix_out,
    G, B1, BX, Kb, Vb, bias, ctx, attp, attt, normed, st, wt, win, wdn,
    xs, xr, xf, rows, actt, pown, psend, precv, ys, ret,
    s1, r1, s2, r2, s3, r3, s4, r4, sb1, rb1, sb2, rb2, sb3, rb3, sb4, rb4,
    kvs, kvr, cxs, cxr, ats, atr, lsem,
    dsem, drem, dloc, fsem, frem, psem, prem, ysem, yrem, yloc,
):
    me = lax.axis_index("seq")
    cs = coords(me)
    y, z, x, core = cs
    bar = pltpu.get_barrier_semaphore()
    sib = dev([y, z, x, 1 - core])

    def signal(i, c):
        pl.semaphore_signal(bar, inc=1, device_id=(lax.rem(me + i, NDEV),), device_id_type=MESH)
        return c

    lax.fori_loop(1, NDEV, signal, 0)
    own = [
        pltpu.make_async_copy(k, Kb.at[8], lsem.at[0]),
        pltpu.make_async_copy(v, Vb.at[8], lsem.at[1]),
    ]
    for c in own:
        c.start()
    weights = [
        pltpu.make_async_copy(w_in, win, lsem.at[2]),
        pltpu.make_async_copy(w_down, wdn, lsem.at[3]),
    ]
    for c in weights:
        c.start()
    for t in range(KT):
        G[y, z, x, t] = w[0:16, t * 128:(t + 1) * 128]
    tail = w[16:20].astype(jnp.float32)
    for i in range(5):
        B1[x, i] = jnp.concatenate(
            [tail[:, n * 640 + i * 128:n * 640 + i * 128 + 128] for n in range(4)], 0
        ).astype(jnp.bfloat16)
    row = lax.broadcasted_iota(jnp.int32, (TOK, TOK), 0)
    col = lax.broadcasted_iota(jnp.int32, (TOK, TOK), 1)
    for j in range(9):
        ok = me - 8 + j >= 0
        if j == 0:
            m = (col > row) & ok
        elif j == 8:
            m = col <= row
        else:
            m = (col >= 0) & ok
        bias[:, j * TOK:(j + 1) * TOK] = jnp.where(m, 0.0, -jnp.inf)
    for c in own:
        c.wait()
    pl.semaphore_wait(bar, NDEV - 1)
    sends = []

    def rc(src, dst, ss, rs, dv):
        c = pltpu.make_async_remote_copy(
            src_ref=src, dst_ref=dst, send_sem=ss, recv_sem=rs, device_id=(dv,), device_id_type=MESH
        )
        c.start()
        sends.append(c)
        return c

    nxt = lax.rem(me + 8, NDEV)
    kv4 = [rc(b_.at[8], b_.at[0], kvs.at[n, 3], kvr.at[n, 3], nxt) for n, b_ in enumerate((Kb, Vb))]
    kvx = []
    for dlt in (1, 2, 3):
        tgt = dev(shift(cs, 2, dlt))
        pair = []
        for n, b_ in enumerate((Kb, Vb)):
            pair.append(
                tuple(
                    pltpu.make_async_remote_copy(
                        src_ref=b_.at[s], dst_ref=b_.at[8 - 2 * dlt], send_sem=kvs.at[n, dlt - 1],
                        recv_sem=kvr.at[n, dlt - 1], device_id=(tgt,), device_id_type=MESH,
                    )
                    for s in (8, 0)
                )
            )
        kvx.append(pair)
        sends += [p_[0] for p_ in pair]

        @pl.when(x + dlt < 4)
        def _():
            for p_ in pair:
                p_[0].start()

    p1 = []
    for pi, ((a, bb, c), t0, tn) in enumerate(PARTS):
        sl = wslice(cs, (), {}, t0, tn)
        p1.append(
            [rc(G.at[sl], G.at[sl], s1.at[pi, i], r1.at[pi, i], dev(shift(cs, a, d))) for i, d in enumerate(DELTAS)]
        )
    pb1 = [rc(B1.at[x], B1.at[x], sb1.at[i], rb1.at[i], dev(shift(cs, 2, d))) for i, d in enumerate(DELTAS)]

    p3 = [[None] * 4 for _ in PARTS]
    pb3 = [None] * 4

    def chunk_send(pi, i, bi):
        (a, bb, c), t0, tn = PARTS[pi]
        sl = wslice(cs, (a,), {bb: bi}, t0, tn)
        p3[pi][i] = [
            rc(G.at[sl], G.at[sl], s3.at[pi, i, n], r3.at[pi, i, n], dev(shift(cs, c, d)))
            for n, d in enumerate(DELTAS[:2])
        ]
        if pi == 0:
            pb3[i] = [
                rc(BX.at[y, bi], BX.at[y, bi], sb3.at[i, n], rb3.at[i, n], dev(shift(cs, 0, d)))
                for n, d in enumerate(DELTAS[:2])
            ]

    p2 = []
    pb2 = []
    for pi, ((a, bb, c), t0, tn) in enumerate(PARTS):
        for n in range(3):
            p1[pi][n].wait_recv()
        if pi == 0:
            for n in range(3):
                pb1[n].wait_recv()
            src = [[B1[xx, i].astype(jnp.float32) for i in range(5)] for xx in range(4)]
            for kq in range(4):
                for i in range(5):
                    BX[y, z, kq * 5 + i] = jnp.concatenate(
                        [src[xx][i][kq * 4:kq * 4 + 4] for xx in range(4)], 0
                    ).astype(jnp.bfloat16)
        sl = wslice(cs, (a,), {}, t0, tn)
        p2.append(
            [rc(G.at[sl], G.at[sl], s2.at[pi, i], r2.at[pi, i], dev(shift(cs, bb, d))) for i, d in enumerate(DELTAS)]
        )
        if pi == 0:
            pb2 = [
                rc(BX.at[y, z], BX.at[y, z], sb2.at[i], rb2.at[i], dev(shift(cs, 1, d)))
                for i, d in enumerate(DELTAS)
            ]
        chunk_send(pi, 0, cs[bb])

    for c in kv4:
        c.wait_recv()
    for dlt in (1, 2, 3):

        @pl.when(x + dlt >= 4)
        def _():
            for p_ in kvx[dlt - 1]:
                p_[1].start()

    for i, d in enumerate(DELTAS):
        for pi, ((a, bb, c), t0, tn) in enumerate(PARTS):
            p2[pi][i].wait_recv()
            if pi == 0:
                pb2[i].wait_recv()
            chunk_send(pi, i + 1, lax.rem(cs[bb] + 4 - d, 4))

    rl = []

    def relay(i):
        for pi, ((a, bb, c), t0, tn) in enumerate(PARTS):
            bi = cs[bb] if i == 0 else lax.rem(cs[bb] + 4 - DELTAS[i - 1], 4)
            h = tn // 2
            for n, (dfrom, dto, lo, cnt) in enumerate(((3, 1, 0, h), (1, 3, h, tn - h))):
                p3[pi][i][n].wait_recv()
                s_ = wslice(cs, (a,), {bb: bi, c: lax.rem(cs[c] + dfrom, 4)}, t0 + lo, cnt)
                rl.append(rc(G.at[s_], G.at[s_], s4.at[pi, i, n], r4.at[pi, i, n], dev(shift(cs, c, dto))))
                if pi == 0:
                    pb3[i][n].wait_recv()
                    b_ = BX.at[lax.rem(y + dfrom, 4), bi, pl.ds(10 * n, 10)]
                    rl.append(rc(b_, b_, sb4.at[i, n], rb4.at[i, n], dev(shift(cs, 0, dto))))

    relay(0)
    routing(routes, gates, modal, cap, st, wt)
    kvd = []
    for p_ in kvx:
        for n in range(2):
            p_[n][0].wait_recv()
    for i in range(4):
        src = 8 - 2 * i - 2 * core
        for n, b_ in enumerate((Kb, Vb)):
            kvd.append(rc(b_.at[src], b_.at[7 - 2 * i], kvs.at[n, 4 + i], kvr.at[n, 4 + i], sib))
    relay(1)
    for c in kvd:
        c.wait_recv()

    scale = HEAD ** (-0.5)
    cxc = []
    for h in range(KV_HEADS):
        hs = slice(h * HEAD, (h + 1) * HEAD)
        kh = Kb[:, :, hs].reshape(9 * TOK, HEAD)
        vh = Vb[:, :, hs].reshape(9 * TOK, HEAD)
        for g in range(GROUP):
            qs = slice((h * GROUP + g) * HEAD, (h * GROUP + g + 1) * HEAD)
            s = lax.dot_general(
                q[:, qs], kh, (((1,), (1,)), ((), ())), preferred_element_type=jnp.float32
            ) * scale + bias[...]
            mx = jnp.max(s, -1, keepdims=True)
            e = jnp.exp(s - mx)
            tot = jnp.sum(e, -1, keepdims=True)
            o = jnp.dot(e.astype(jnp.bfloat16), vh, preferred_element_type=jnp.float32)
            ctx[core, h, :, g * HEAD:(g + 1) * HEAD] = (o / tot).astype(jnp.bfloat16)
        cxc.append(rc(ctx.at[core, h], ctx.at[core, h], cxs.at[h], cxr.at[h], sib))
        if h < 2:
            relay(h + 2)
    for c in cxc:
        c.wait_recv()
    for c in rl:
        c.wait_recv()

    def project(tile_pair):
        acc = None
        for kp in range(KT // 2):
            lhs = tile_pair(2 * kp)
            h, off = (2 * kp) // GROUP, (2 * kp) % GROUP
            cols = []
            for t in (2 * kp, 2 * kp + 1):
                hh, oo = t // GROUP, t % GROUP
                cols.append(ctx[:, hh, :, oo * HEAD:(oo + 1) * HEAD].reshape(2 * TOK, HEAD))
            rhs = jnp.concatenate(cols, 1)
            part = lax.dot_general(lhs, rhs, (((1,), (1,)), ((), ())), preferred_element_type=jnp.float32)
            acc = part if acc is None else acc + part
        return acc.astype(jnp.bfloat16)

    def put(first, rows, val):
        attp[core, 0, pl.ds(first, rows)] = val[:, :TOK]
        attp[core, 1, pl.ds(first, rows)] = val[:, TOK:]

    def a_rows(yy, carry):
        def pair(t):
            return jnp.concatenate(
                [G[yy, :, :, t + i].reshape(256, 128) for i in range(2)], 1
            )
        put(yy * 256, 256, project(pair))
        return carry

    lax.fori_loop(0, 4, a_rows, 0)
    put(1024, 256, project(
        lambda t: jnp.concatenate([BX[:, :, t + i].reshape(256, 128) for i in range(2)], 1)
    ))
    xc = rc(attp.at[core, 1 - core], attp.at[core, 1 - core], ats, atr, sib)
    xc.wait_recv()
    mine = [attp.at[0, core], attp.at[1, core]]
    for chip in range(64):
        for c in range(2):
            d0 = 20 * (chip * 2 + c)
            attt[d0:d0 + 16] = mine[c][chip * 16:chip * 16 + 16].astype(jnp.float32)
    for yz in range(16):
        for c in range(2):
            blk = mine[c][1024 + yz * 16:1024 + yz * 16 + 16].astype(jnp.float32)
            for xx in range(4):
                d0 = 20 * ((yz * 4 + xx) * 2 + c) + 16
                attt[d0:d0 + 4] = blk[xx * 4:xx * 4 + 4]
    ssq = jnp.zeros((TOK, 1), jnp.float32)
    for t in range(KT):
        ls = slice(t * 128, (t + 1) * 128)
        a_ = jnp.transpose(attt[ls])
        att_out[:, ls] = a_.astype(jnp.bfloat16)
        hd = res[:, ls].astype(jnp.float32) + a_
        ssq = ssq + jnp.sum(hd * hd, -1, keepdims=True)
    inv = lax.rsqrt(ssq / D + 1e-05)
    for t in range(KT):
        ls = slice(t * 128, (t + 1) * 128)
        hd = res[:, ls].astype(jnp.float32) + att_out[:, ls].astype(jnp.float32)
        normed[:, ls] = (hd * inv * gain[ls][None, :]).astype(jnp.bfloat16)

    xs[...] = jnp.dot(st[...], normed[...], preferred_element_type=jnp.float32).astype(
        jnp.bfloat16
    ).reshape(NDEV, CAP, D)
    mine = pltpu.make_async_copy(xs.at[me], xr.at[0], dloc)
    mine.start()
    HALF = NDEV // 2

    def offset(i, sign):
        off = order(i)
        full = [4, 4, 4, 2]
        return dev([lax.rem(cs[n] + (off[n] if sign > 0 else full[n] - off[n]), full[n]) for n in range(4)])

    def send_half(half):
        def send(i, c):
            t = offset(i, 1)
            pltpu.make_async_remote_copy(
                src_ref=xs.at[t], dst_ref=xr.at[i], send_sem=dsem.at[half], recv_sem=drem.at[half],
                device_id=(t,), device_id_type=MESH,
            ).start()
            return c

        lax.fori_loop(max(1, half * HALF), (half + 1) * HALF, send, 0)

    send_half(0)
    send_half(1)
    mine.wait()

    def whole(src, dst, half, ss, rs):
        n = HALF - 1 if half == 0 else HALF
        part = pl.ds(half * HALF, n)
        return pltpu.make_async_remote_copy(
            src_ref=src.at[part], dst_ref=dst.at[part], send_sem=ss.at[half], recv_sem=rs.at[half],
            device_id=(sib,), device_id_type=MESH,
        )

    for c in weights:
        c.wait()
    fwd, back = [], []

    def arrive(half):
        whole(xs, xr, half, dsem, drem).wait_recv()
        part = pl.ds(half * HALF, HALF)
        fwd.append(rc(xr.at[part], xf.at[part], fsem.at[half], frem.at[half], sib))
        rows[:TOK] = xr[part].reshape(TOK, D)
        fwd[half].wait_recv()
        rows[TOK:] = xf[part].reshape(TOK, D)

    def experts(half):
        def hidden(n, c):
            at = pl.ds(pl.multiple_of(n * 208, 16), 208)
            nt = (((1,), (1,)), ((), ()))
            gate = lax.dot_general(win[0, at], rows[...], nt, preferred_element_type=jnp.float32)
            up = lax.dot_general(win[1, at], rows[...], nt, preferred_element_type=jnp.float32)
            actt[at] = (gate * lax.logistic(gate) * up).astype(jnp.bfloat16)
            return c

        lax.fori_loop(0, 4, hidden, 0)
        act = jnp.transpose(actt[...].astype(jnp.float32)).astype(jnp.bfloat16)
        for n in range(2):
            ls = pl.ds(n * 1280, 1280)
            psend[half, :, ls] = jnp.dot(
                act[TOK:], wdn[:, ls], preferred_element_type=jnp.float32
            ).astype(jnp.bfloat16)
        back.append(rc(psend.at[half], precv.at[half], psem.at[half], prem.at[half], sib))
        for n in range(2):
            ls = pl.ds(n * 1280, 1280)
            pown[:, ls] = jnp.dot(
                act[:TOK], wdn[:, ls], preferred_element_type=jnp.float32
            ).astype(jnp.bfloat16)

    def give(half):
        back[half].wait_recv()
        part = pl.ds(half * HALF, HALF)
        ys[part] = (
            pown[...].astype(jnp.float32) + precv[half].astype(jnp.float32)
        ).astype(jnp.bfloat16).reshape(HALF, CAP, D)

        def send(i, c):
            t = offset(i, -1)
            pltpu.make_async_remote_copy(
                src_ref=ys.at[i], dst_ref=ret.at[me], send_sem=ysem.at[half], recv_sem=yrem.at[0],
                device_id=(t,), device_id_type=MESH,
            ).start()
            return c

        lax.fori_loop(max(1, half * HALF), (half + 1) * HALF, send, 0)

    arrive(0)
    experts(0)
    give(0)
    home = pltpu.make_async_copy(ys.at[0], ret.at[me], yloc)
    home.start()
    arrive(1)
    experts(1)
    give(1)
    home.wait()
    for half in range(2):
        whole(xs, xr, half, dsem, drem).wait_send()
        whole(ys, ret, half, ysem, ysem).wait_send()
    every = pl.ds(0, NDEV - 1)
    pltpu.make_async_remote_copy(
        src_ref=ys.at[every], dst_ref=ret.at[every], send_sem=ysem.at[0], recv_sem=yrem.at[0],
        device_id=(sib,), device_id_type=MESH,
    ).wait_recv()
    back_rows = ret[...].reshape(2 * NDEV, D)
    mix = jnp.dot(wt[0], back_rows, preferred_element_type=jnp.float32) + jnp.dot(
        wt[1], back_rows, preferred_element_type=jnp.float32
    )
    mix_out[...] = (mix * (1.0 / 1024.0)).astype(jnp.bfloat16)
    for c in sends:
        c.wait_send()


def body(
    residual, queries, keys, values, out_proj, norm_gain, expert_in, expert_down,
    routes, gate_ints, modality, capacity,
):
    any_ = pl.BlockSpec(memory_space=pl.ANY)
    vm = pl.BlockSpec(memory_space=pltpu.VMEM)
    bf = jnp.bfloat16
    cols = expert_in.shape[2]
    return pl.pallas_call(
        layer_kernel,
        out_shape=(jax.ShapeDtypeStruct((TOK, D), bf), jax.ShapeDtypeStruct((TOK, D), bf)),
        in_specs=[vm, vm, any_, any_, vm, vm, any_, any_, vm, vm, vm, vm],
        out_specs=(vm, vm),
        scratch_shapes=[
            pltpu.VMEM((4, 4, 4, KT, 16, 128), bf),
            pltpu.VMEM((4, 5, 16, 128), bf),
            pltpu.VMEM((4, 4, KT, 16, 128), bf),
            pltpu.VMEM((9, TOK, KV_HEADS * HEAD), bf),
            pltpu.VMEM((9, TOK, KV_HEADS * HEAD), bf),
            pltpu.VMEM((TOK, 9 * TOK), jnp.float32),
            pltpu.VMEM((2, KV_HEADS, TOK, GROUP * HEAD), bf),
            pltpu.VMEM((2, 2, 1280, TOK), bf),
            pltpu.VMEM((D, TOK), jnp.float32),
            pltpu.VMEM((TOK, D), bf),
            pltpu.VMEM((2 * NDEV, TOK), bf),
            pltpu.VMEM((2, TOK, 2 * NDEV), bf),
            pltpu.VMEM((2, cols, D), bf),
            pltpu.VMEM((cols, D), bf),
            pltpu.VMEM((NDEV, CAP, D), bf),
            pltpu.VMEM((NDEV, CAP, D), bf),
            pltpu.VMEM((NDEV, CAP, D), bf),
            pltpu.VMEM((2 * TOK, D), bf),
            pltpu.VMEM((cols, 2 * TOK), bf),
            pltpu.VMEM((TOK, D), bf),
            pltpu.VMEM((2, TOK, D), bf),
            pltpu.VMEM((2, TOK, D), bf),
            pltpu.VMEM((NDEV, CAP, D), bf),
            pltpu.VMEM((NDEV, CAP, D), bf),
            DMA((3, 3)), DMA((3, 3)), DMA((3, 3)), DMA((3, 3)),
            DMA((3, 4, 2)), DMA((3, 4, 2)), DMA((3, 4, 2)), DMA((3, 4, 2)),
            DMA((3,)), DMA((3,)), DMA((3,)), DMA((3,)),
            DMA((4, 2)), DMA((4, 2)), DMA((4, 2)), DMA((4, 2)),
            DMA((2, 8)), DMA((2, 8)), DMA((4,)), DMA((4,)), DMA, DMA, DMA((4,)),
            DMA((2,)), DMA((2,)), DMA, DMA((2,)), DMA((2,)), DMA((2,)), DMA((2,)), DMA((2,)), DMA((1,)), DMA,
        ],
        compiler_params=pltpu.CompilerParams(
            has_side_effects=True, collective_id=0, vmem_limit_bytes=60 * 2**20
        ),
    )(
        out_proj.T, queries, keys, values, residual, norm_gain, expert_in.transpose(1, 2, 0), expert_down,
        routes.T, gate_ints.T, modality, capacity.T,
    )


def solution(mesh):
    placed = (
        P("seq", None), P("seq", None), P("seq", None), P("seq", None), P(None, "seq"), P(),
        P(None, None, "seq"), P("seq", None), P("seq", None), P("seq", None), P("seq"), P(),
    )
    return jax.shard_map(
        body, mesh=mesh, in_specs=placed, out_specs=(P("seq", None), P("seq", None)), check_vma=False
    )
```

```python
import functools

import jax
import jax.numpy as jnp
from jax import lax
from jax.experimental import pallas as pl
from jax.experimental.pallas import tpu as pltpu
from jax.sharding import PartitionSpec as P

HEADS = 20
KV_HEADS = 4
HEAD = 128
GROUP = HEADS // KV_HEADS
WINDOW = 1024
EXPERTS = 64
CAP = 2
D = 2560
TOK = 128
NDEV = 128
MESH = pl.DeviceIdType.MESH
DMA = pltpu.SemaphoreType.DMA
DELTAS = (1, 3, 2)
PARTS = (((2, 1, 0), 0, 5), ((1, 0, 2), 5, 6), ((2, 0, 1), 11, 9))
KT = D // 128


def coords(me):
    return [me // 32, (me // 8) % 4, (me // 2) % 4, me % 2]


def dev(cs):
    return ((cs[0] * 4 + cs[1]) * 4 + cs[2]) * 2 + cs[3]


def shift(cs, dim, d):
    cs = list(cs)
    cs[dim] = lax.rem(cs[dim] + d, 4)
    return cs


def wslice(cs, alld, fixed, t0, tn):
    idx = [slice(None) if d in alld else cs[d] for d in range(3)]
    for d, v in fixed.items():
        idx[d] = v
    return tuple(idx) + (pl.ds(t0, tn),)


def order(i):
    s = (i * 37) % NDEV
    return [s // 32, (s // 8) % 4, (s // 2) % 4, s % 2]


def routing(routes, gates, modal, cap, st, wt):
    rows = 2 * NDEV
    rho = lax.broadcasted_iota(jnp.int32, (rows, TOK), 0)
    key, turn = jnp.right_shift(rho, 1), jnp.bitwise_and(rho, 1)
    mod = modal[...][None, :]
    is0 = key == routes[0:1] * 2 + mod
    is1 = key == routes[1:2] * 2 + mod
    hit = jnp.where(is0 | is1, 1.0, 0.0)
    before = lax.broadcasted_iota(jnp.int32, (TOK, TOK), 0) < lax.broadcasted_iota(jnp.int32, (TOK, TOK), 1)
    rank = jnp.dot(
        hit.astype(jnp.bfloat16), jnp.where(before, 1.0, 0.0).astype(jnp.bfloat16),
        preferred_element_type=jnp.float32,
    )
    rho_e = lax.broadcasted_iota(jnp.int32, (rows, EXPERTS), 0)
    at_e = lax.broadcasted_iota(jnp.int32, (rows, EXPERTS), 1) == jnp.right_shift(rho_e, 2)
    cap_e = jnp.where(jnp.bitwise_and(rho_e, 2) == 0, cap[0:1], cap[1:2]).astype(jnp.float32)
    limit = jnp.sum(jnp.where(at_e, cap_e, 0.0), -1, keepdims=True)
    turn_f = turn.astype(jnp.float32)
    kept = jnp.where((rank == turn_f) & (turn_f < limit), hit, 0.0)
    st[...] = kept.astype(jnp.bfloat16)
    g = jnp.where(is0, gates[0:1], gates[1:2])
    high = jnp.bitwise_and(g, 1016)
    wt[0] = jnp.transpose(high.astype(jnp.float32) * kept).astype(jnp.bfloat16)
    wt[1] = jnp.transpose((g - high).astype(jnp.float32) * kept).astype(jnp.bfloat16)


def layer_kernel(
    w, q, k, v, res, gain, w_in, w_down, routes, gates, modal, cap, att_out, mix_out,
    G, B1, BX, Ko, Vo, Kb, Vb, qb, bias, ctx, attp, attt, normed, st, wt, win, wdn,
    xs, xr, xf, rows, actt, pown, psend, precv, ys, ret,
    s1, r1, s2, r2, s3, r3, s4, r4, sb1, rb1, sb2, rb2, sb3, rb3, sb4, rb4,
    kzs, kzr, kxs, kxr, kds, kdr, cxs, cxr, ats, atr, lsem,
    dsem, drem, dloc, fsem, frem, psem, prem, ysem, yrem, yloc,
):
    me = lax.axis_index("seq")
    cs = coords(me)
    y, z, x, core = cs
    bar = pltpu.get_barrier_semaphore()
    sib = dev([y, z, x, 1 - core])

    def signal(i, c):
        pl.semaphore_signal(bar, inc=1, device_id=(lax.rem(me + i, NDEV),), device_id_type=MESH)
        return c

    lax.fori_loop(1, NDEV, signal, 0)
    half_w = KV_HEADS * HEAD // 2
    own = []
    for n, (src, own_, buf) in enumerate(((k, Ko, Kb), (v, Vo, Vb))):
        for hf in range(2):
            own.append(pltpu.make_async_copy(src.at[:, pl.ds(hf * half_w, half_w)], own_.at[hf], lsem.at[3 * n + hf]))
        own.append(pltpu.make_async_copy(
            src.at[:, pl.ds(pl.multiple_of(core * half_w, half_w), half_w)], buf.at[8 + core], lsem.at[3 * n + 2]
        ))
    for c in own:
        c.start()
    weights = [
        pltpu.make_async_copy(w_in, win, lsem.at[6]),
        pltpu.make_async_copy(w_down, wdn, lsem.at[7]),
    ]
    for c in weights:
        c.start()
    for t in range(KT):
        G[y, z, x, t] = w[0:16, t * 128:(t + 1) * 128]
    tail = w[16:20].astype(jnp.float32)
    for i in range(5):
        B1[x, i] = jnp.concatenate(
            [tail[:, n * 640 + i * 128:n * 640 + i * 128 + 128] for n in range(4)], 0
        ).astype(jnp.bfloat16)
    row = lax.broadcasted_iota(jnp.int32, (TOK, TOK), 0)
    col = lax.broadcasted_iota(jnp.int32, (TOK, TOK), 1)
    for p in range(2):
        for j in range(9):
            ok = me - core - 8 + j + p >= 0
            if j == 0:
                m = (col > row) & ok
            elif j == 8:
                m = col <= row
            else:
                m = (col >= 0) & ok
            bias[p, :, j * TOK:(j + 1) * TOK] = jnp.where(m, 0.0, -jnp.inf)
    mine_q = pl.ds(pl.multiple_of(core * (D // 2), 128), D // 2)
    qb[core] = q[:, mine_q]
    for c in own:
        c.wait()
    pl.semaphore_wait(bar, NDEV - 1)
    sends = []

    def rc(src, dst, ss, rs, dv):
        c = pltpu.make_async_remote_copy(
            src_ref=src, dst_ref=dst, send_sem=ss, recv_sem=rs, device_id=(dv,), device_id_type=MESH
        )
        c.start()
        sends.append(c)
        return c

    p1 = []
    for pi, ((a, bb, c), t0, tn) in enumerate(PARTS):
        sl = wslice(cs, (), {}, t0, tn)
        p1.append(
            [rc(G.at[sl], G.at[sl], s1.at[pi, i], r1.at[pi, i], dev(shift(cs, a, d))) for i, d in enumerate(DELTAS)]
        )
    pb1 = [rc(B1.at[x], B1.at[x], sb1.at[i], rb1.at[i], dev(shift(cs, 2, d))) for i, d in enumerate(DELTAS)]

    def twin(cs_, c_):
        return dev(cs_[:3] + [c_])

    kvz, kvx, kvx_wait = [], [], []
    up = lax.rem(me - core + 8, NDEV)
    for n, (own_, buf) in enumerate(((Ko, Kb), (Vo, Vb))):
        for hf in range(2):
            kvz.append(rc(own_.at[hf], buf.at[core], kzs.at[n, hf], kzr.at[n, core], up + hf))
    qx = rc(q.at[:, pl.ds(pl.multiple_of((1 - core) * (D // 2), 128), D // 2)], qb.at[core], cxs.at[4], cxr.at[4], sib)
    kvd = [
        rc(own_.at[1 - core], buf.at[8 + core], kds.at[n], kdr.at[n], sib)
        for n, (own_, buf) in enumerate(((Ko, Kb), (Vo, Vb)))
    ]
    for dlt in (1, 3, 2):
        tgt = shift(cs, 2, dlt)
        for n, (own_, buf) in enumerate(((Ko, Kb), (Vo, Vb))):
            for hf in range(2):
                slot = (4 - dlt) * 2
                fresh = pltpu.make_async_remote_copy(
                    src_ref=own_.at[hf], dst_ref=buf.at[slot + core], send_sem=kxs.at[n, dlt - 1, hf],
                    recv_sem=kxr.at[n, dlt - 1, core], device_id=(twin(tgt, hf),), device_id_type=MESH,
                )
                older = pltpu.make_async_remote_copy(
                    src_ref=buf.at[hf], dst_ref=buf.at[slot + hf], send_sem=kxs.at[n, dlt - 1, hf],
                    recv_sem=kxr.at[n, dlt - 1, hf], device_id=(twin(tgt, core),), device_id_type=MESH,
                )
                kvx.append((n, dlt, fresh, older))
                kvx_wait.append(older)

    for n, dlt, fresh, older in kvx:
        sends.append(older)

        @pl.when(x + dlt < 4)
        def _():
            fresh.start()

    p3 = [[None] * 4 for _ in PARTS]
    pb3 = [None] * 4

    def chunk_send(pi, i, bi):
        (a, bb, c), t0, tn = PARTS[pi]
        sl = wslice(cs, (a,), {bb: bi}, t0, tn)
        p3[pi][i] = [
            rc(G.at[sl], G.at[sl], s3.at[pi, i, n], r3.at[pi, i, n], dev(shift(cs, c, d)))
            for n, d in enumerate(DELTAS[:2])
        ]
        if pi == 0:
            pb3[i] = [
                rc(BX.at[y, bi], BX.at[y, bi], sb3.at[i, n], rb3.at[i, n], dev(shift(cs, 0, d)))
                for n, d in enumerate(DELTAS[:2])
            ]

    p2 = [None] * 3
    pb2 = []
    for pi in (0, 2, 1):
        (a, bb, c), t0, tn = PARTS[pi]
        for n in range(3):
            p1[pi][n].wait_recv()
        if pi == 0:
            for n in range(3):
                pb1[n].wait_recv()
            src = [[B1[xx, i].astype(jnp.float32) for i in range(5)] for xx in range(4)]
            for kq in range(4):
                for i in range(5):
                    BX[y, z, kq * 5 + i] = jnp.concatenate(
                        [src[xx][i][kq * 4:kq * 4 + 4] for xx in range(4)], 0
                    ).astype(jnp.bfloat16)
        sl = wslice(cs, (a,), {}, t0, tn)
        p2[pi] = [
            rc(G.at[sl], G.at[sl], s2.at[pi, i], r2.at[pi, i], dev(shift(cs, bb, d))) for i, d in enumerate(DELTAS)
        ]
        if pi == 0:
            pb2 = [
                rc(BX.at[y, z], BX.at[y, z], sb2.at[i], rb2.at[i], dev(shift(cs, 1, d)))
                for i, d in enumerate(DELTAS)
            ]
        chunk_send(pi, 0, cs[bb])

    for n, buf in enumerate((Kb, Vb)):
        for hf in range(2):
            pltpu.make_async_remote_copy(
                src_ref=buf.at[hf], dst_ref=buf.at[hf], send_sem=kzs.at[n, hf], recv_sem=kzr.at[n, hf],
                device_id=(up,), device_id_type=MESH,
            ).wait_recv()
        for n_, dlt, fresh, older in kvx:
            if n_ == n:

                @pl.when(x + dlt >= 4)
                def _():
                    older.start()

    for i, d in enumerate(DELTAS):
        for pi, ((a, bb, c), t0, tn) in enumerate(PARTS):
            p2[pi][i].wait_recv()
            if pi == 0:
                pb2[i].wait_recv()
            chunk_send(pi, i + 1, lax.rem(cs[bb] + 4 - d, 4))

    rl = []

    def relay(i):
        for pi, ((a, bb, c), t0, tn) in enumerate(PARTS):
            bi = cs[bb] if i == 0 else lax.rem(cs[bb] + 4 - DELTAS[i - 1], 4)
            h = tn // 2
            for n, (dfrom, dto, lo, cnt) in enumerate(((3, 1, 0, h), (1, 3, h, tn - h))):
                p3[pi][i][n].wait_recv()
                s_ = wslice(cs, (a,), {bb: bi, c: lax.rem(cs[c] + dfrom, 4)}, t0 + lo, cnt)
                rl.append(rc(G.at[s_], G.at[s_], s4.at[pi, i, n], r4.at[pi, i, n], dev(shift(cs, c, dto))))
                if pi == 0:
                    pb3[i][n].wait_recv()
                    b_ = BX.at[lax.rem(y + dfrom, 4), bi, pl.ds(10 * n, 10)]
                    rl.append(rc(b_, b_, sb4.at[i, n], rb4.at[i, n], dev(shift(cs, 0, dto))))

    relay(0)
    routing(routes, gates, modal, cap, st, wt)
    relay(1)
    for c in kvd + kvx_wait:
        c.wait_recv()
    qx.wait_recv()

    scale = HEAD ** (-0.5)
    cxc = []
    for hl in range(2):
        hs = slice(hl * HEAD, (hl + 1) * HEAD)
        h = 2 * core + hl
        for p in range(2):
            kh = Kb[p:p + 9, :, hs].reshape(9 * TOK, HEAD)
            vh = Vb[p:p + 9, :, hs].reshape(9 * TOK, HEAD)
            for g in range(GROUP):
                qs = slice((hl * GROUP + g) * HEAD, (hl * GROUP + g + 1) * HEAD)
                s = lax.dot_general(
                    qb[p, :, qs], kh, (((1,), (1,)), ((), ())), preferred_element_type=jnp.float32
                ) * scale + bias[p]
                mx = jnp.max(s, -1, keepdims=True)
                e = jnp.exp(s - mx)
                tot = jnp.sum(e, -1, keepdims=True)
                o = jnp.dot(e.astype(jnp.bfloat16), vh, preferred_element_type=jnp.float32)
                ctx[p, h, :, g * HEAD:(g + 1) * HEAD] = (o / tot).astype(jnp.bfloat16)
            cxc.append(rc(ctx.at[p, h], ctx.at[p, h], cxs.at[2 * hl + p], cxr.at[2 * hl + p], sib))
            if p == 1:
                relay(hl + 2)
    for c in cxc:
        c.wait_recv()
    for c in rl:
        c.wait_recv()

    def project(tile_pair):
        acc = None
        for kp in range(KT // 2):
            lhs = tile_pair(2 * kp)
            h, off = (2 * kp) // GROUP, (2 * kp) % GROUP
            cols = []
            for t in (2 * kp, 2 * kp + 1):
                hh, oo = t // GROUP, t % GROUP
                cols.append(ctx[:, hh, :, oo * HEAD:(oo + 1) * HEAD].reshape(2 * TOK, HEAD))
            rhs = jnp.concatenate(cols, 1)
            part = lax.dot_general(lhs, rhs, (((1,), (1,)), ((), ())), preferred_element_type=jnp.float32)
            acc = part if acc is None else acc + part
        return acc.astype(jnp.bfloat16)

    def put(first, rows, val):
        attp[core, 0, pl.ds(first, rows)] = val[:, :TOK]
        attp[core, 1, pl.ds(first, rows)] = val[:, TOK:]

    def a_rows(yy, carry):
        def pair(t):
            return jnp.concatenate(
                [G[yy, :, :, t + i].reshape(256, 128) for i in range(2)], 1
            )
        put(yy * 256, 256, project(pair))
        return carry

    lax.fori_loop(0, 4, a_rows, 0)
    put(1024, 256, project(
        lambda t: jnp.concatenate([BX[:, :, t + i].reshape(256, 128) for i in range(2)], 1)
    ))
    xc = rc(attp.at[core, 1 - core], attp.at[core, 1 - core], ats, atr, sib)
    xc.wait_recv()
    mine = [attp.at[0, core], attp.at[1, core]]
    for chip in range(64):
        for c in range(2):
            d0 = 20 * (chip * 2 + c)
            attt[d0:d0 + 16] = mine[c][chip * 16:chip * 16 + 16].astype(jnp.float32)
    for yz in range(16):
        for c in range(2):
            blk = mine[c][1024 + yz * 16:1024 + yz * 16 + 16].astype(jnp.float32)
            for xx in range(4):
                d0 = 20 * ((yz * 4 + xx) * 2 + c) + 16
                attt[d0:d0 + 4] = blk[xx * 4:xx * 4 + 4]
    ssq = jnp.zeros((TOK, 1), jnp.float32)
    for t in range(KT):
        ls = slice(t * 128, (t + 1) * 128)
        a_ = jnp.transpose(attt[ls])
        att_out[:, ls] = a_.astype(jnp.bfloat16)
        hd = res[:, ls].astype(jnp.float32) + a_
        ssq = ssq + jnp.sum(hd * hd, -1, keepdims=True)
    inv = lax.rsqrt(ssq / D + 1e-05)
    for t in range(KT):
        ls = slice(t * 128, (t + 1) * 128)
        hd = res[:, ls].astype(jnp.float32) + att_out[:, ls].astype(jnp.float32)
        normed[:, ls] = (hd * inv * gain[ls][None, :]).astype(jnp.bfloat16)

    xs[...] = jnp.dot(st[...], normed[...], preferred_element_type=jnp.float32).astype(
        jnp.bfloat16
    ).reshape(NDEV, CAP, D)
    mine = pltpu.make_async_copy(xs.at[me], xr.at[0], dloc)
    mine.start()
    HALF = NDEV // 2

    def offset(i, sign):
        off = order(i)
        full = [4, 4, 4, 2]
        return dev([lax.rem(cs[n] + (off[n] if sign > 0 else full[n] - off[n]), full[n]) for n in range(4)])

    def send_half(half):
        def send(i, c):
            t = offset(i, 1)
            pltpu.make_async_remote_copy(
                src_ref=xs.at[t], dst_ref=xr.at[i], send_sem=dsem.at[half], recv_sem=drem.at[half],
                device_id=(t,), device_id_type=MESH,
            ).start()
            return c

        lax.fori_loop(max(1, half * HALF), (half + 1) * HALF, send, 0)

    send_half(0)
    send_half(1)
    mine.wait()

    def whole(src, dst, half, ss, rs):
        n = HALF - 1 if half == 0 else HALF
        part = pl.ds(half * HALF, n)
        return pltpu.make_async_remote_copy(
            src_ref=src.at[part], dst_ref=dst.at[part], send_sem=ss.at[half], recv_sem=rs.at[half],
            device_id=(sib,), device_id_type=MESH,
        )

    for c in weights:
        c.wait()
    fwd, back = [], []

    def arrive(half):
        whole(xs, xr, half, dsem, drem).wait_recv()
        part = pl.ds(half * HALF, HALF)
        fwd.append(rc(xr.at[part], xf.at[part], fsem.at[half], frem.at[half], sib))
        rows[:TOK] = xr[part].reshape(TOK, D)
        fwd[half].wait_recv()
        rows[TOK:] = xf[part].reshape(TOK, D)

    def experts(half):
        def hidden(n, c):
            at = pl.ds(pl.multiple_of(n * 208, 16), 208)
            nt = (((1,), (1,)), ((), ()))
            gate = lax.dot_general(win[0, at], rows[...], nt, preferred_element_type=jnp.float32)
            up = lax.dot_general(win[1, at], rows[...], nt, preferred_element_type=jnp.float32)
            actt[at] = (gate * lax.logistic(gate) * up).astype(jnp.bfloat16)
            return c

        lax.fori_loop(0, 4, hidden, 0)
        act = jnp.transpose(actt[...].astype(jnp.float32)).astype(jnp.bfloat16)
        for n in range(2):
            ls = pl.ds(n * 1280, 1280)
            psend[half, :, ls] = jnp.dot(
                act[TOK:], wdn[:, ls], preferred_element_type=jnp.float32
            ).astype(jnp.bfloat16)
        back.append(rc(psend.at[half], precv.at[half], psem.at[half], prem.at[half], sib))
        for n in range(2):
            ls = pl.ds(n * 1280, 1280)
            pown[:, ls] = jnp.dot(
                act[:TOK], wdn[:, ls], preferred_element_type=jnp.float32
            ).astype(jnp.bfloat16)

    def give(half):
        back[half].wait_recv()
        part = pl.ds(half * HALF, HALF)
        ys[part] = (
            pown[...].astype(jnp.float32) + precv[half].astype(jnp.float32)
        ).astype(jnp.bfloat16).reshape(HALF, CAP, D)

        def send(i, c):
            t = offset(i, -1)
            pltpu.make_async_remote_copy(
                src_ref=ys.at[i], dst_ref=ret.at[me], send_sem=ysem.at[half], recv_sem=yrem.at[0],
                device_id=(t,), device_id_type=MESH,
            ).start()
            return c

        lax.fori_loop(max(1, half * HALF), (half + 1) * HALF, send, 0)

    arrive(0)
    experts(0)
    give(0)
    home = pltpu.make_async_copy(ys.at[0], ret.at[me], yloc)
    home.start()
    arrive(1)
    experts(1)
    give(1)
    home.wait()
    for half in range(2):
        whole(xs, xr, half, dsem, drem).wait_send()
        whole(ys, ret, half, ysem, ysem).wait_send()
    every = pl.ds(0, NDEV - 1)
    pltpu.make_async_remote_copy(
        src_ref=ys.at[every], dst_ref=ret.at[every], send_sem=ysem.at[0], recv_sem=yrem.at[0],
        device_id=(sib,), device_id_type=MESH,
    ).wait_recv()
    back_rows = ret[...].reshape(2 * NDEV, D)
    mix = jnp.dot(wt[0], back_rows, preferred_element_type=jnp.float32) + jnp.dot(
        wt[1], back_rows, preferred_element_type=jnp.float32
    )
    mix_out[...] = (mix * (1.0 / 1024.0)).astype(jnp.bfloat16)
    for c in sends:
        c.wait_send()


def out_kernel(a, b, a_out, b_out, sem):
    copies = [pltpu.make_async_copy(a, a_out, sem.at[0]), pltpu.make_async_copy(b, b_out, sem.at[1])]
    for c in copies:
        c.start()
    for c in copies:
        c.wait()


def body(
    residual, queries, keys, values, out_proj, norm_gain, expert_in, expert_down,
    routes, gate_ints, modality, capacity,
):
    any_ = pl.BlockSpec(memory_space=pl.ANY)
    vm = pl.BlockSpec(memory_space=pltpu.VMEM)
    bf = jnp.bfloat16
    cols = expert_in.shape[2]
    outs = pl.pallas_call(
        layer_kernel,
        out_shape=(jax.ShapeDtypeStruct((TOK, D), bf), jax.ShapeDtypeStruct((TOK, D), bf)),
        in_specs=[vm, vm, any_, any_, vm, vm, any_, any_, vm, vm, vm, vm],
        out_specs=(vm, vm),
        scratch_shapes=[
            pltpu.VMEM((4, 4, 4, KT, 16, 128), bf),
            pltpu.VMEM((4, 5, 16, 128), bf),
            pltpu.VMEM((4, 4, KT, 16, 128), bf),
            pltpu.VMEM((2, TOK, KV_HEADS * HEAD // 2), bf),
            pltpu.VMEM((2, TOK, KV_HEADS * HEAD // 2), bf),
            pltpu.VMEM((10, TOK, KV_HEADS * HEAD // 2), bf),
            pltpu.VMEM((10, TOK, KV_HEADS * HEAD // 2), bf),
            pltpu.VMEM((2, TOK, D // 2), bf),
            pltpu.VMEM((2, TOK, 9 * TOK), jnp.float32),
            pltpu.VMEM((2, KV_HEADS, TOK, GROUP * HEAD), bf),
            pltpu.VMEM((2, 2, 1280, TOK), bf),
            pltpu.VMEM((D, TOK), jnp.float32),
            pltpu.VMEM((TOK, D), bf),
            pltpu.VMEM((2 * NDEV, TOK), bf),
            pltpu.VMEM((2, TOK, 2 * NDEV), bf),
            pltpu.VMEM((2, cols, D), bf),
            pltpu.VMEM((cols, D), bf),
            pltpu.VMEM((NDEV, CAP, D), bf),
            pltpu.VMEM((NDEV, CAP, D), bf),
            pltpu.VMEM((NDEV, CAP, D), bf),
            pltpu.VMEM((2 * TOK, D), bf),
            pltpu.VMEM((cols, 2 * TOK), bf),
            pltpu.VMEM((TOK, D), bf),
            pltpu.VMEM((2, TOK, D), bf),
            pltpu.VMEM((2, TOK, D), bf),
            pltpu.VMEM((NDEV, CAP, D), bf),
            pltpu.VMEM((NDEV, CAP, D), bf),
            DMA((3, 3)), DMA((3, 3)), DMA((3, 3)), DMA((3, 3)),
            DMA((3, 4, 2)), DMA((3, 4, 2)), DMA((3, 4, 2)), DMA((3, 4, 2)),
            DMA((3,)), DMA((3,)), DMA((3,)), DMA((3,)),
            DMA((4, 2)), DMA((4, 2)), DMA((4, 2)), DMA((4, 2)),
            DMA((2, 2)), DMA((2, 2)), DMA((2, 3, 2)), DMA((2, 3, 2)), DMA((2,)), DMA((2,)),
            DMA((5,)), DMA((5,)), DMA, DMA, DMA((8,)),
            DMA((2,)), DMA((2,)), DMA, DMA((2,)), DMA((2,)), DMA((2,)), DMA((2,)), DMA((2,)), DMA((1,)), DMA,
        ],
        compiler_params=pltpu.CompilerParams(
            has_side_effects=True, collective_id=0, vmem_limit_bytes=60 * 2**20
        ),
    )(
        out_proj.T, queries, keys, values, residual, norm_gain, expert_in.transpose(1, 2, 0), expert_down,
        routes.T, gate_ints.T, modality, capacity.T,
    )
    shape = jax.ShapeDtypeStruct((TOK, D), bf)
    return pl.pallas_call(
        out_kernel, out_shape=(shape, shape), in_specs=[vm, vm], out_specs=(any_, any_), scratch_shapes=[DMA((2,))],
        compiler_params=pltpu.CompilerParams(vmem_limit_bytes=4 * 2**20),
    )(*outs)


def solution(mesh):
    placed = (
        P("seq", None), P("seq", None), P("seq", None), P("seq", None), P(None, "seq"), P(),
        P(None, None, "seq"), P("seq", None), P("seq", None), P("seq", None), P("seq"), P(),
    )
    return jax.shard_map(
        body, mesh=mesh, in_specs=placed, out_specs=(P("seq", None), P("seq", None)), check_vma=False
    )
```

```python
import functools

import jax
import jax.numpy as jnp
from jax import lax
from jax.experimental import pallas as pl
from jax.experimental.pallas import tpu as pltpu
from jax.sharding import PartitionSpec as P

HEADS = 20
KV_HEADS = 4
HEAD = 128
GROUP = HEADS // KV_HEADS
WINDOW = 1024
EXPERTS = 64
CAP = 2
D = 2560
TOK = 128
NDEV = 128
MESH = pl.DeviceIdType.MESH
DMA = pltpu.SemaphoreType.DMA
DELTAS = (1, 3, 2)
PARTS = (((2, 1, 0), 0, 4), ((1, 0, 2), 4, 8), ((2, 0, 1), 12, 8))
CHUNKS = ((0, 64), (64, 64))
KT = D // 128


def coords(me):
    return [me // 32, (me // 8) % 4, (me // 2) % 4, me % 2]


def dev(cs):
    return ((cs[0] * 4 + cs[1]) * 4 + cs[2]) * 2 + cs[3]


def shift(cs, dim, d):
    cs = list(cs)
    cs[dim] = lax.rem(cs[dim] + d, 4)
    return cs


def wslice(cs, alld, fixed, t0, tn):
    idx = [slice(None) if d in alld else cs[d] for d in range(3)]
    for d, v in fixed.items():
        idx[d] = v
    return tuple(idx) + (pl.ds(t0, tn),)


def order(i):
    s = (i * 59) % NDEV
    return [s // 32, (s // 8) % 4, (s // 2) % 4, s % 2]


def routing(routes, gates, modal, cap, st, wt):
    rows = 2 * NDEV
    rho = lax.broadcasted_iota(jnp.int32, (rows, TOK), 0)
    key, turn = jnp.right_shift(rho, 1), jnp.bitwise_and(rho, 1)
    mod = modal[...][None, :]
    is0 = key == routes[0:1] * 2 + mod
    is1 = key == routes[1:2] * 2 + mod
    hit = jnp.where(is0 | is1, 1.0, 0.0)
    before = lax.broadcasted_iota(jnp.int32, (TOK, TOK), 0) < lax.broadcasted_iota(jnp.int32, (TOK, TOK), 1)
    rank = jnp.dot(
        hit.astype(jnp.bfloat16), jnp.where(before, 1.0, 0.0).astype(jnp.bfloat16),
        preferred_element_type=jnp.float32,
    )
    rho_e = lax.broadcasted_iota(jnp.int32, (rows, EXPERTS), 0)
    at_e = lax.broadcasted_iota(jnp.int32, (rows, EXPERTS), 1) == jnp.right_shift(rho_e, 2)
    cap_e = jnp.where(jnp.bitwise_and(rho_e, 2) == 0, cap[0:1], cap[1:2]).astype(jnp.float32)
    limit = jnp.sum(jnp.where(at_e, cap_e, 0.0), -1, keepdims=True)
    turn_f = turn.astype(jnp.float32)
    kept = jnp.where((rank == turn_f) & (turn_f < limit), hit, 0.0)
    st[...] = kept.astype(jnp.bfloat16)
    g = jnp.where(is0, gates[0:1], gates[1:2])
    high = jnp.bitwise_and(g, 1016)
    wt[0] = jnp.transpose(high.astype(jnp.float32) * kept).astype(jnp.bfloat16)
    wt[1] = jnp.transpose((g - high).astype(jnp.float32) * kept).astype(jnp.bfloat16)


def layer_kernel(
    w, q, k, v, res, gain, w_in, w_down, routes, gates, modal, cap, att_out, mix_out,
    G, B1, BX, Ko, Vo, Kb, Vb, qb, bias, ctx, attp, attt, normed, st, wt, win, wdn,
    xs, xr, xf, rows, pown, psend, precv, ys, ret,
    s1, r1, s2, r2, s3, r3, s4, r4, sb1, rb1, sb2, rb2, sb3, rb3, sb4, rb4,
    kzs, kzr, kxs, kxr, kds, kdr, cxs, cxr, ats, atr, lsem,
    dsem, drem, dloc, fsem, frem, psem, prem, ysem, yrem, yloc,
):
    me = lax.axis_index("seq")
    cs = coords(me)
    y, z, x, core = cs
    bar = pltpu.get_barrier_semaphore()
    sib = dev([y, z, x, 1 - core])

    def signal(i, c):
        pl.semaphore_signal(bar, inc=1, device_id=(lax.rem(me + i, NDEV),), device_id_type=MESH)
        return c

    lax.fori_loop(1, NDEV, signal, 0)
    half_w = KV_HEADS * HEAD // 2
    own = []
    for n, (src, own_, buf) in enumerate(((k, Ko, Kb), (v, Vo, Vb))):
        for hf in range(2):
            own.append(pltpu.make_async_copy(src.at[:, pl.ds(hf * half_w, half_w)], own_.at[hf], lsem.at[3 * n + hf]))
        own.append(pltpu.make_async_copy(
            src.at[:, pl.ds(pl.multiple_of(core * half_w, half_w), half_w)], buf.at[8 + core], lsem.at[3 * n + 2]
        ))
    for c in own:
        c.start()
    weights = [
        pltpu.make_async_copy(w_in, win, lsem.at[6]),
        pltpu.make_async_copy(w_down, wdn, lsem.at[7]),
    ]
    for c in weights:
        c.start()
    for t in range(KT):
        G[y, z, x, t] = w[0:16, t * 128:(t + 1) * 128]
    tail = w[16:20].astype(jnp.float32)
    for i in range(5):
        B1[x, i] = jnp.concatenate(
            [tail[:, n * 640 + i * 128:n * 640 + i * 128 + 128] for n in range(4)], 0
        ).astype(jnp.bfloat16)
    key_at = lax.broadcasted_iota(jnp.int32, (TOK, TOK), 0)
    query_at = lax.broadcasted_iota(jnp.int32, (TOK, TOK), 1)
    for p in range(2):
        for j in range(9):
            ok = me - core - 8 + j + p >= 0
            if j == 0:
                m = (key_at > query_at) & ok
            elif j == 8:
                m = key_at <= query_at
            else:
                m = (key_at >= 0) & ok
            bias[p, j * TOK:(j + 1) * TOK] = jnp.where(m, 0.0, -jnp.inf)
    mine_q = pl.ds(pl.multiple_of(core * (D // 2), 128), D // 2)
    qb[core] = q[:, mine_q]
    for c in own:
        c.wait()
    pl.semaphore_wait(bar, NDEV - 1)
    sends = []

    def rc(src, dst, ss, rs, dv):
        c = pltpu.make_async_remote_copy(
            src_ref=src, dst_ref=dst, send_sem=ss, recv_sem=rs, device_id=(dv,), device_id_type=MESH
        )
        c.start()
        sends.append(c)
        return c

    p1 = []
    for pi, ((a, bb, c), t0, tn) in enumerate(PARTS):
        sl = wslice(cs, (), {}, t0, tn)
        p1.append(
            [rc(G.at[sl], G.at[sl], s1.at[pi, i], r1.at[pi, i], dev(shift(cs, a, d))) for i, d in enumerate(DELTAS)]
        )
    pb1 = [rc(B1.at[x], B1.at[x], sb1.at[i], rb1.at[i], dev(shift(cs, 2, d))) for i, d in enumerate(DELTAS)]

    def twin(cs_, c_):
        return dev(cs_[:3] + [c_])

    kvz, kvx, kvx_wait = [], [], []
    up = lax.rem(me - core + 8, NDEV)
    for n, (own_, buf) in enumerate(((Ko, Kb), (Vo, Vb))):
        for hf in range(2):
            kvz.append(rc(own_.at[hf], buf.at[core], kzs.at[n, hf], kzr.at[n, core], up + hf))
    qx = rc(q.at[:, pl.ds(pl.multiple_of((1 - core) * (D // 2), 128), D // 2)], qb.at[core], cxs.at[4], cxr.at[4], sib)
    kvd = [
        rc(own_.at[1 - core], buf.at[8 + core], kds.at[n], kdr.at[n], sib)
        for n, (own_, buf) in enumerate(((Ko, Kb), (Vo, Vb)))
    ]
    for dlt in (1, 3, 2):
        tgt = shift(cs, 2, dlt)
        for n, (own_, buf) in enumerate(((Ko, Kb), (Vo, Vb))):
            for hf in range(2):
                slot = (4 - dlt) * 2
                fresh = pltpu.make_async_remote_copy(
                    src_ref=own_.at[hf], dst_ref=buf.at[slot + core], send_sem=kxs.at[n, dlt - 1, hf],
                    recv_sem=kxr.at[n, dlt - 1, core], device_id=(twin(tgt, hf),), device_id_type=MESH,
                )
                older = pltpu.make_async_remote_copy(
                    src_ref=buf.at[hf], dst_ref=buf.at[slot + hf], send_sem=kxs.at[n, dlt - 1, hf],
                    recv_sem=kxr.at[n, dlt - 1, hf], device_id=(twin(tgt, core),), device_id_type=MESH,
                )
                kvx.append((n, dlt, fresh, older))
                kvx_wait.append(older)

    for n, dlt, fresh, older in kvx:
        sends.append(older)

        @pl.when(x + dlt < 4)
        def _():
            fresh.start()

    p3 = [[None] * 4 for _ in PARTS]
    pb3 = [None] * 4

    def chunk_send(pi, i, bi):
        (a, bb, c), t0, tn = PARTS[pi]
        sl = wslice(cs, (a,), {bb: bi}, t0, tn)
        p3[pi][i] = [
            rc(G.at[sl], G.at[sl], s3.at[pi, i, n], r3.at[pi, i, n], dev(shift(cs, c, d)))
            for n, d in enumerate(DELTAS[:3 if i == 3 else 2])
        ]
        if pi == 0:
            pb3[i] = [
                rc(BX.at[y, bi], BX.at[y, bi], sb3.at[i, n], rb3.at[i, n], dev(shift(cs, 0, d)))
                for n, d in enumerate(DELTAS[:3 if i == 3 else 2])
            ]

    p2 = [None] * 3
    pb2 = []
    for pi in (0, 2, 1):
        (a, bb, c), t0, tn = PARTS[pi]
        for n in range(3):
            p1[pi][n].wait_recv()
        if pi == 0:
            for n in range(3):
                pb1[n].wait_recv()
            src = [[B1[xx, i].astype(jnp.float32) for i in range(5)] for xx in range(4)]
            for kq in range(4):
                for i in range(5):
                    BX[y, z, kq * 5 + i] = jnp.concatenate(
                        [src[xx][i][kq * 4:kq * 4 + 4] for xx in range(4)], 0
                    ).astype(jnp.bfloat16)
        sl = wslice(cs, (a,), {}, t0, tn)
        p2[pi] = [
            rc(G.at[sl], G.at[sl], s2.at[pi, i], r2.at[pi, i], dev(shift(cs, bb, d))) for i, d in enumerate(DELTAS)
        ]
        if pi == 0:
            pb2 = [
                rc(BX.at[y, z], BX.at[y, z], sb2.at[i], rb2.at[i], dev(shift(cs, 1, d)))
                for i, d in enumerate(DELTAS)
            ]
        chunk_send(pi, 0, cs[bb])

    for n, buf in enumerate((Kb, Vb)):
        for hf in range(2):
            pltpu.make_async_remote_copy(
                src_ref=buf.at[hf], dst_ref=buf.at[hf], send_sem=kzs.at[n, hf], recv_sem=kzr.at[n, hf],
                device_id=(up,), device_id_type=MESH,
            ).wait_recv()
        for n_, dlt, fresh, older in kvx:
            if n_ == n:

                @pl.when(x + dlt >= 4)
                def _():
                    older.start()

    for i, d in enumerate(DELTAS):
        for pi, ((a, bb, c), t0, tn) in enumerate(PARTS):
            p2[pi][i].wait_recv()
            if pi == 0:
                pb2[i].wait_recv()
            chunk_send(pi, i + 1, lax.rem(cs[bb] + 4 - d, 4))

    rl = []

    def relay(i):
        for pi, ((a, bb, c), t0, tn) in enumerate(PARTS):
            bi = cs[bb] if i == 0 else lax.rem(cs[bb] + 4 - DELTAS[i - 1], 4)
            h = tn // 2
            for n, (dfrom, dto, lo, cnt) in enumerate(((3, 1, 0, h), (1, 3, h, tn - h))):
                p3[pi][i][n].wait_recv()
                s_ = wslice(cs, (a,), {bb: bi, c: lax.rem(cs[c] + dfrom, 4)}, t0 + lo, cnt)
                rl.append(rc(G.at[s_], G.at[s_], s4.at[pi, i, n], r4.at[pi, i, n], dev(shift(cs, c, dto))))
                if pi == 0:
                    pb3[i][n].wait_recv()
                    b_ = BX.at[lax.rem(y + dfrom, 4), bi, pl.ds(10 * n, 10)]
                    rl.append(rc(b_, b_, sb4.at[i, n], rb4.at[i, n], dev(shift(cs, 0, dto))))

    relay(0)
    routing(routes, gates, modal, cap, st, wt)
    relay(1)
    for c in kvd + kvx_wait:
        c.wait_recv()
    qx.wait_recv()

    scale = HEAD ** (-0.5)
    cxc = []
    for hl in range(2):
        hs = slice(hl * HEAD, (hl + 1) * HEAD)
        first_col = (2 * core + hl) * GROUP
        vt = jnp.transpose(Vb[:, :, hs].reshape(10 * TOK, HEAD).astype(jnp.float32)).astype(jnp.bfloat16)
        for p in range(2):
            kh = Kb[p:p + 9, :, hs].reshape(9 * TOK, HEAD)
            heads = [qb[p, :, (hl * GROUP + g) * HEAD:(hl * GROUP + g + 1) * HEAD] for g in range(GROUP)]
            st_ = lax.dot_general(
                kh, jnp.concatenate(heads, 0), (((1,), (1,)), ((), ())), preferred_element_type=jnp.float32
            ) * scale + jnp.concatenate([bias[p]] * GROUP, 1)
            e = jnp.exp(st_ - jnp.max(st_, 0, keepdims=True))
            tot = jnp.sum(e, 0, keepdims=True)
            o = jnp.dot(
                vt[:, p * TOK:(p + 9) * TOK], e.astype(jnp.bfloat16), preferred_element_type=jnp.float32
            ) / tot
            for g in range(GROUP):
                ctx[first_col + g, :, p * TOK:(p + 1) * TOK] = o[:, g * TOK:(g + 1) * TOK].astype(jnp.bfloat16)
            ready = ctx.at[pl.ds(first_col, GROUP), :, pl.ds(p * TOK, TOK)]
            cxc.append(rc(ready, ready, cxs.at[2 * hl + p], cxr.at[2 * hl + p], sib))
            if hl == 0 and p == 0:
                relay(2)
    for c in cxc:
        c.wait_recv()
    for c in rl + pb3[3] + p3[0][3] + p3[1][3] + p3[2][3]:
        c.wait_recv()

    def project(tile_pair):
        acc = None
        for kp in range(KT // 2):
            rhs = ctx[2 * kp:2 * kp + 2].reshape(2 * HEAD, 2 * TOK)
            part = jnp.dot(tile_pair(2 * kp), rhs, preferred_element_type=jnp.float32)
            acc = part if acc is None else acc + part
        return acc.astype(jnp.bfloat16)

    def put(first, rows, val):
        attp[core, 0, pl.ds(first, rows)] = val[:, :TOK]
        attp[core, 1, pl.ds(first, rows)] = val[:, TOK:]

    def a_rows(yy, carry):
        def pair(t):
            return jnp.concatenate(
                [G[yy, :, :, t + i].reshape(256, 128) for i in range(2)], 1
            )
        put(yy * 256, 256, project(pair))
        return carry

    lax.fori_loop(0, 4, a_rows, 0)
    put(1024, 256, project(
        lambda t: jnp.concatenate([BX[:, :, t + i].reshape(256, 128) for i in range(2)], 1)
    ))
    xc = rc(attp.at[core, 1 - core], attp.at[core, 1 - core], ats, atr, sib)
    xc.wait_recv()
    mine = [attp.at[0, core], attp.at[1, core]]
    for chip in range(64):
        for c in range(2):
            d0 = 20 * (chip * 2 + c)
            attt[d0:d0 + 16] = mine[c][chip * 16:chip * 16 + 16].astype(jnp.float32)
    for yz in range(16):
        for c in range(2):
            blk = mine[c][1024 + yz * 16:1024 + yz * 16 + 16].astype(jnp.float32)
            for xx in range(4):
                d0 = 20 * ((yz * 4 + xx) * 2 + c) + 16
                attt[d0:d0 + 4] = blk[xx * 4:xx * 4 + 4]
    ssq = jnp.zeros((TOK, 1), jnp.float32)
    for t in range(KT):
        ls = slice(t * 128, (t + 1) * 128)
        a_ = jnp.transpose(attt[ls])
        att_out[:, ls] = a_.astype(jnp.bfloat16)
        hd = res[:, ls].astype(jnp.float32) + a_
        ssq = ssq + jnp.sum(hd * hd, -1, keepdims=True)
    inv = lax.rsqrt(ssq / D + 1e-05)
    for t in range(KT):
        ls = slice(t * 128, (t + 1) * 128)
        hd = res[:, ls].astype(jnp.float32) + att_out[:, ls].astype(jnp.float32)
        normed[:, ls] = (hd * inv * gain[ls][None, :]).astype(jnp.bfloat16)

    xs[...] = jnp.dot(st[...], normed[...], preferred_element_type=jnp.float32).astype(
        jnp.bfloat16
    ).reshape(NDEV, CAP, D)
    mine = pltpu.make_async_copy(xs.at[me], xr.at[0], dloc)
    mine.start()

    def offset(i, sign):
        off = order(i)
        full = [4, 4, 4, 2]
        return dev([lax.rem(cs[n] + (off[n] if sign > 0 else full[n] - off[n]), full[n]) for n in range(4)])

    for ch, (first, size) in enumerate(CHUNKS):

        def send(i, c):
            t = offset(i, 1)
            pltpu.make_async_remote_copy(
                src_ref=xs.at[t], dst_ref=xr.at[i], send_sem=dsem.at[ch], recv_sem=drem.at[ch],
                device_id=(t,), device_id_type=MESH,
            ).start()
            return c

        lax.fori_loop(max(1, first), first + size, send, 0)
    mine.wait()

    def whole(src, dst, ch, ss, rs):
        first, size = CHUNKS[ch]
        part = pl.ds(first, size - 1 if first == 0 else size)
        return pltpu.make_async_remote_copy(
            src_ref=src.at[part], dst_ref=dst.at[part], send_sem=ss.at[ch], recv_sem=rs.at[ch],
            device_id=(sib,), device_id_type=MESH,
        )

    for c in weights:
        c.wait()
    nt = (((1,), (1,)), ((), ()))
    home = pltpu.make_async_copy(ys.at[0], ret.at[me], yloc)
    for ch, (first, size) in enumerate(CHUNKS):
        part = pl.ds(first, size)
        flat = pl.ds(first * CAP, size * CAP)
        count = size * CAP
        whole(xs, xr, ch, dsem, drem).wait_recv()
        fwd = rc(xr.at[part], xf.at[part], fsem.at[ch], frem.at[ch], sib)
        rows[:count] = xr[part].reshape(count, D)
        fwd.wait_recv()
        rows[count:2 * count] = xf[part].reshape(count, D)
        both = rows[:2 * count]
        gate = lax.dot_general(win[0], both, nt, preferred_element_type=jnp.float32)
        up = lax.dot_general(win[1], both, nt, preferred_element_type=jnp.float32)
        act = jnp.transpose(gate * lax.logistic(gate) * up).astype(jnp.bfloat16)
        psend[flat] = jnp.dot(act[count:], wdn[...], preferred_element_type=jnp.float32).astype(jnp.bfloat16)
        back = rc(psend.at[flat], precv.at[flat], psem.at[ch], prem.at[ch], sib)
        pown[:count] = jnp.dot(act[:count], wdn[...], preferred_element_type=jnp.float32).astype(jnp.bfloat16)
        back.wait_recv()
        ys[part] = (
            pown[:count].astype(jnp.float32) + precv[flat].astype(jnp.float32)
        ).astype(jnp.bfloat16).reshape(size, CAP, D)

        def give(i, c):
            t = offset(i, -1)
            pltpu.make_async_remote_copy(
                src_ref=ys.at[i], dst_ref=ret.at[me], send_sem=ysem.at[ch], recv_sem=yrem.at[0],
                device_id=(t,), device_id_type=MESH,
            ).start()
            return c

        lax.fori_loop(max(1, first), first + size, give, 0)
        if ch == 0:
            home.start()
    home.wait()
    for ch in range(len(CHUNKS)):
        whole(xs, xr, ch, dsem, drem).wait_send()
        whole(ys, ret, ch, ysem, ysem).wait_send()
    every = pl.ds(0, NDEV - 1)
    pltpu.make_async_remote_copy(
        src_ref=ys.at[every], dst_ref=ret.at[every], send_sem=ysem.at[0], recv_sem=yrem.at[0],
        device_id=(sib,), device_id_type=MESH,
    ).wait_recv()
    back_rows = ret[...].reshape(2 * NDEV, D)
    mix = jnp.dot(wt[0], back_rows, preferred_element_type=jnp.float32) + jnp.dot(
        wt[1], back_rows, preferred_element_type=jnp.float32
    )
    mix_out[...] = (mix * (1.0 / 1024.0)).astype(jnp.bfloat16)
    for c in sends:
        c.wait_send()


def out_kernel(a, b, a_out, b_out, sem):
    copies = [pltpu.make_async_copy(a, a_out, sem.at[0]), pltpu.make_async_copy(b, b_out, sem.at[1])]
    for c in copies:
        c.start()
    for c in copies:
        c.wait()


def body(
    residual, queries, keys, values, out_proj, norm_gain, expert_in, expert_down,
    routes, gate_ints, modality, capacity,
):
    any_ = pl.BlockSpec(memory_space=pl.ANY)
    vm = pl.BlockSpec(memory_space=pltpu.VMEM)
    bf = jnp.bfloat16
    cols = expert_in.shape[2]
    outs = pl.pallas_call(
        layer_kernel,
        out_shape=(jax.ShapeDtypeStruct((TOK, D), bf), jax.ShapeDtypeStruct((TOK, D), bf)),
        in_specs=[vm, vm, any_, any_, vm, vm, any_, any_, vm, vm, vm, vm],
        out_specs=(vm, vm),
        scratch_shapes=[
            pltpu.VMEM((4, 4, 4, KT, 16, 128), bf),
            pltpu.VMEM((4, 5, 16, 128), bf),
            pltpu.VMEM((4, 4, KT, 16, 128), bf),
            pltpu.VMEM((2, TOK, KV_HEADS * HEAD // 2), bf),
            pltpu.VMEM((2, TOK, KV_HEADS * HEAD // 2), bf),
            pltpu.VMEM((10, TOK, KV_HEADS * HEAD // 2), bf),
            pltpu.VMEM((10, TOK, KV_HEADS * HEAD // 2), bf),
            pltpu.VMEM((2, TOK, D // 2), bf),
            pltpu.VMEM((2, 9 * TOK, TOK), jnp.float32),
            pltpu.VMEM((KT, HEAD, 2 * TOK), bf),
            pltpu.VMEM((2, 2, 1280, TOK), bf),
            pltpu.VMEM((D, TOK), jnp.float32),
            pltpu.VMEM((TOK, D), bf),
            pltpu.VMEM((2 * NDEV, TOK), bf),
            pltpu.VMEM((2, TOK, 2 * NDEV), bf),
            pltpu.VMEM((2, cols, D), bf),
            pltpu.VMEM((cols, D), bf),
            pltpu.VMEM((NDEV, CAP, D), bf),
            pltpu.VMEM((NDEV, CAP, D), bf),
            pltpu.VMEM((NDEV, CAP, D), bf),
            pltpu.VMEM((2 * TOK, D), bf),
            pltpu.VMEM((TOK, D), bf),
            pltpu.VMEM((2 * TOK, D), bf),
            pltpu.VMEM((2 * TOK, D), bf),
            pltpu.VMEM((NDEV, CAP, D), bf),
            pltpu.VMEM((NDEV, CAP, D), bf),
            DMA((3, 3)), DMA((3, 3)), DMA((3, 3)), DMA((3, 3)),
            DMA((3, 4, 3)), DMA((3, 4, 3)), DMA((3, 4, 2)), DMA((3, 4, 2)),
            DMA((3,)), DMA((3,)), DMA((3,)), DMA((3,)),
            DMA((4, 3)), DMA((4, 3)), DMA((4, 2)), DMA((4, 2)),
            DMA((2, 2)), DMA((2, 2)), DMA((2, 3, 2)), DMA((2, 3, 2)), DMA((2,)), DMA((2,)),
            DMA((5,)), DMA((5,)), DMA, DMA, DMA((8,)),
            DMA((3,)), DMA((3,)), DMA, DMA((3,)), DMA((3,)), DMA((3,)), DMA((3,)), DMA((3,)), DMA((1,)), DMA,
        ],
        compiler_params=pltpu.CompilerParams(
            has_side_effects=True, collective_id=0, vmem_limit_bytes=60 * 2**20
        ),
    )(
        out_proj.T, queries, keys, values, residual, norm_gain, expert_in.transpose(1, 2, 0), expert_down,
        routes.T, gate_ints.T, modality, capacity.T,
    )
    shape = jax.ShapeDtypeStruct((TOK, D), bf)
    return pl.pallas_call(
        out_kernel, out_shape=(shape, shape), in_specs=[vm, vm], out_specs=(any_, any_), scratch_shapes=[DMA((2,))],
        compiler_params=pltpu.CompilerParams(vmem_limit_bytes=4 * 2**20),
    )(*outs)


def solution(mesh):
    placed = (
        P("seq", None), P("seq", None), P("seq", None), P("seq", None), P(None, "seq"), P(),
        P(None, None, "seq"), P("seq", None), P("seq", None), P("seq", None), P("seq"), P(),
    )
    return jax.shard_map(
        body, mesh=mesh, in_specs=placed, out_specs=(P("seq", None), P("seq", None)), check_vma=False
    )
```

```python
import functools

import jax
import jax.numpy as jnp
from jax import lax
from jax.experimental import pallas as pl
from jax.experimental.pallas import tpu as pltpu
from jax.sharding import PartitionSpec as P

HEADS = 20
KV_HEADS = 4
HEAD = 128
GROUP = HEADS // KV_HEADS
WINDOW = 1024
EXPERTS = 64
CAP = 2
D = 2560
TOK = 128
NDEV = 128
MESH = pl.DeviceIdType.MESH
DMA = pltpu.SemaphoreType.DMA
DELTAS = (1, 3, 2)
PARTS = (((2, 1, 0), 0, 4), ((1, 0, 2), 4, 8), ((2, 0, 1), 12, 8))
CHUNKS = ((0, 64), (64, 64))
KT = D // 128


def coords(me):
    return [me // 32, (me // 8) % 4, (me // 2) % 4, me % 2]


def dev(cs):
    return ((cs[0] * 4 + cs[1]) * 4 + cs[2]) * 2 + cs[3]


def shift(cs, dim, d):
    cs = list(cs)
    cs[dim] = lax.rem(cs[dim] + d, 4)
    return cs


def wslice(cs, alld, fixed, t0, tn):
    idx = [slice(None) if d in alld else cs[d] for d in range(3)]
    for d, v in fixed.items():
        idx[d] = v
    return tuple(idx) + (pl.ds(t0, tn),)


def order(i):
    s = (i * 59) % NDEV
    return [s // 32, (s // 8) % 4, (s // 2) % 4, s % 2]


def routing(cs, routes, gates, modal, cap, st, wt):
    rows = 2 * NDEV
    rho = lax.broadcasted_iota(jnp.int32, (rows, TOK), 0)
    turn = jnp.bitwise_and(rho, 1)

    def device(at):
        off = jnp.bitwise_and(jnp.right_shift(at, 1) * 59, NDEV - 1)
        y, z, x, core = cs
        ny = jnp.bitwise_and(y + jnp.right_shift(off, 5), 3)
        nz = jnp.bitwise_and(z + jnp.bitwise_and(jnp.right_shift(off, 3), 3), 3)
        nx = jnp.bitwise_and(x + jnp.bitwise_and(jnp.right_shift(off, 1), 3), 3)
        return ny * 32 + nz * 8 + nx * 2 + jnp.bitwise_and(core + off, 1)

    key = device(rho)
    mod = modal[...][None, :]
    is0 = key == routes[0:1] * 2 + mod
    is1 = key == routes[1:2] * 2 + mod
    hit = jnp.where(is0 | is1, 1.0, 0.0)
    before = lax.broadcasted_iota(jnp.int32, (TOK, TOK), 0) < lax.broadcasted_iota(jnp.int32, (TOK, TOK), 1)
    rank = jnp.dot(
        hit.astype(jnp.bfloat16), jnp.where(before, 1.0, 0.0).astype(jnp.bfloat16),
        preferred_element_type=jnp.float32,
    )
    key_e = device(lax.broadcasted_iota(jnp.int32, (rows, EXPERTS), 0))
    at_e = lax.broadcasted_iota(jnp.int32, (rows, EXPERTS), 1) == jnp.right_shift(key_e, 1)
    cap_e = jnp.where(jnp.bitwise_and(key_e, 1) == 0, cap[0:1], cap[1:2]).astype(jnp.float32)
    limit = jnp.sum(jnp.where(at_e, cap_e, 0.0), -1, keepdims=True)
    turn_f = turn.astype(jnp.float32)
    kept = jnp.where((rank == turn_f) & (turn_f < limit), hit, 0.0)
    st[...] = kept.astype(jnp.bfloat16)
    g = jnp.where(is0, gates[0:1], gates[1:2])
    high = jnp.bitwise_and(g, 1016)
    wt[0] = jnp.transpose(high.astype(jnp.float32) * kept).astype(jnp.bfloat16)
    wt[1] = jnp.transpose((g - high).astype(jnp.float32) * kept).astype(jnp.bfloat16)


def layer_kernel(
    w, q, k, v, res, gain, w_in, w_down, routes, gates, modal, cap, att_out, mix_out,
    G, B1, BX, Ko, Vo, Kb, Vb, qb, bias, ctx, attp, attt, normed, st, wt, win, wdn,
    xs, xr, xf, rows, pown, psend, precv, ys, ret,
    s1, r1, s2, r2, s3, r3, s4, r4, sb1, rb1, sb2, rb2, sb3, rb3, sb4, rb4,
    kzs, kzr, kxs, kxr, kds, kdr, cxs, cxr, ats, atr, lsem,
    dsem, drem, dloc, fsem, frem, psem, prem, ysem, yrem, yloc,
):
    me = lax.axis_index("seq")
    cs = coords(me)
    y, z, x, core = cs
    bar = pltpu.get_barrier_semaphore()
    sib = dev([y, z, x, 1 - core])

    def signal(i, c):
        pl.semaphore_signal(bar, inc=1, device_id=(lax.rem(me + i, NDEV),), device_id_type=MESH)
        return c

    lax.fori_loop(1, NDEV, signal, 0)
    half_w = KV_HEADS * HEAD // 2
    own = []
    for n, (src, own_, buf) in enumerate(((k, Ko, Kb), (v, Vo, Vb))):
        for hf in range(2):
            own.append(pltpu.make_async_copy(src.at[:, pl.ds(hf * half_w, half_w)], own_.at[hf], lsem.at[3 * n + hf]))
        own.append(pltpu.make_async_copy(
            src.at[:, pl.ds(pl.multiple_of(core * half_w, half_w), half_w)], buf.at[8 + core], lsem.at[3 * n + 2]
        ))
    for c in own:
        c.start()
    weights = [
        pltpu.make_async_copy(w_in, win, lsem.at[6]),
        pltpu.make_async_copy(w_down, wdn, lsem.at[7]),
    ]
    for c in weights:
        c.start()
    for t in range(KT):
        G[y, z, x, t] = w[0:16, t * 128:(t + 1) * 128]
    tail = w[16:20].astype(jnp.float32)
    for i in range(5):
        B1[x, i] = jnp.concatenate(
            [tail[:, n * 640 + i * 128:n * 640 + i * 128 + 128] for n in range(4)], 0
        ).astype(jnp.bfloat16)
    key_at = lax.broadcasted_iota(jnp.int32, (TOK, TOK), 0)
    query_at = lax.broadcasted_iota(jnp.int32, (TOK, TOK), 1)
    for p in range(2):
        for j in range(9):
            ok = me - core - 8 + j + p >= 0
            if j == 0:
                m = (key_at > query_at) & ok
            elif j == 8:
                m = key_at <= query_at
            else:
                m = (key_at >= 0) & ok
            bias[p, j * TOK:(j + 1) * TOK] = jnp.where(m, 0.0, -jnp.inf)
    mine_q = pl.ds(pl.multiple_of(core * (D // 2), 128), D // 2)
    qb[core] = q[:, mine_q]
    for c in own:
        c.wait()
    pl.semaphore_wait(bar, NDEV - 1)
    sends = []

    def rc(src, dst, ss, rs, dv):
        c = pltpu.make_async_remote_copy(
            src_ref=src, dst_ref=dst, send_sem=ss, recv_sem=rs, device_id=(dv,), device_id_type=MESH
        )
        c.start()
        sends.append(c)
        return c

    p1 = []
    for pi, ((a, bb, c), t0, tn) in enumerate(PARTS):
        sl = wslice(cs, (), {}, t0, tn)
        p1.append(
            [rc(G.at[sl], G.at[sl], s1.at[pi, i], r1.at[pi, i], dev(shift(cs, a, d))) for i, d in enumerate(DELTAS)]
        )
    pb1 = [rc(B1.at[x], B1.at[x], sb1.at[i], rb1.at[i], dev(shift(cs, 2, d))) for i, d in enumerate(DELTAS)]

    def twin(cs_, c_):
        return dev(cs_[:3] + [c_])

    kvz, kvx, kvx_wait = [], [], []
    up = lax.rem(me - core + 8, NDEV)
    for n, (own_, buf) in enumerate(((Ko, Kb), (Vo, Vb))):
        for hf in range(2):
            kvz.append(rc(own_.at[hf], buf.at[core], kzs.at[n, hf], kzr.at[n, core], up + hf))
    qx = rc(q.at[:, pl.ds(pl.multiple_of((1 - core) * (D // 2), 128), D // 2)], qb.at[core], cxs.at[4], cxr.at[4], sib)
    kvd = [
        rc(own_.at[1 - core], buf.at[8 + core], kds.at[n], kdr.at[n], sib)
        for n, (own_, buf) in enumerate(((Ko, Kb), (Vo, Vb)))
    ]
    for dlt in (1, 3, 2):
        tgt = shift(cs, 2, dlt)
        for n, (own_, buf) in enumerate(((Ko, Kb), (Vo, Vb))):
            for hf in range(2):
                slot = (4 - dlt) * 2
                fresh = pltpu.make_async_remote_copy(
                    src_ref=own_.at[hf], dst_ref=buf.at[slot + core], send_sem=kxs.at[n, dlt - 1, hf],
                    recv_sem=kxr.at[n, dlt - 1, core], device_id=(twin(tgt, hf),), device_id_type=MESH,
                )
                older = pltpu.make_async_remote_copy(
                    src_ref=buf.at[hf], dst_ref=buf.at[slot + hf], send_sem=kxs.at[n, dlt - 1, hf],
                    recv_sem=kxr.at[n, dlt - 1, hf], device_id=(twin(tgt, core),), device_id_type=MESH,
                )
                kvx.append((n, dlt, fresh, older))
                kvx_wait.append(older)

    for n, dlt, fresh, older in kvx:
        sends.append(older)

        @pl.when(x + dlt < 4)
        def _():
            fresh.start()

    p3 = [[None] * 4 for _ in PARTS]
    pb3 = [None] * 4

    def chunk_send(pi, i, bi):
        (a, bb, c), t0, tn = PARTS[pi]
        sl = wslice(cs, (a,), {bb: bi}, t0, tn)
        p3[pi][i] = [
            rc(G.at[sl], G.at[sl], s3.at[pi, i, n], r3.at[pi, i, n], dev(shift(cs, c, d)))
            for n, d in enumerate(DELTAS[:3 if i == 3 else 2])
        ]
        if pi == 0:
            pb3[i] = [
                rc(BX.at[y, bi], BX.at[y, bi], sb3.at[i, n], rb3.at[i, n], dev(shift(cs, 0, d)))
                for n, d in enumerate(DELTAS[:3 if i == 3 else 2])
            ]

    p2 = [None] * 3
    pb2 = []
    for pi in (0, 2, 1):
        (a, bb, c), t0, tn = PARTS[pi]
        for n in range(3):
            p1[pi][n].wait_recv()
        if pi == 0:
            for n in range(3):
                pb1[n].wait_recv()
            src = [[B1[xx, i].astype(jnp.float32) for i in range(5)] for xx in range(4)]
            for kq in range(4):
                for i in range(5):
                    BX[y, z, kq * 5 + i] = jnp.concatenate(
                        [src[xx][i][kq * 4:kq * 4 + 4] for xx in range(4)], 0
                    ).astype(jnp.bfloat16)
        sl = wslice(cs, (a,), {}, t0, tn)
        p2[pi] = [
            rc(G.at[sl], G.at[sl], s2.at[pi, i], r2.at[pi, i], dev(shift(cs, bb, d))) for i, d in enumerate(DELTAS)
        ]
        if pi == 0:
            pb2 = [
                rc(BX.at[y, z], BX.at[y, z], sb2.at[i], rb2.at[i], dev(shift(cs, 1, d)))
                for i, d in enumerate(DELTAS)
            ]
        chunk_send(pi, 0, cs[bb])

    for n, buf in enumerate((Kb, Vb)):
        for hf in range(2):
            pltpu.make_async_remote_copy(
                src_ref=buf.at[hf], dst_ref=buf.at[hf], send_sem=kzs.at[n, hf], recv_sem=kzr.at[n, hf],
                device_id=(up,), device_id_type=MESH,
            ).wait_recv()
        for n_, dlt, fresh, older in kvx:
            if n_ == n:

                @pl.when(x + dlt >= 4)
                def _():
                    older.start()

    for i, d in enumerate(DELTAS):
        for pi, ((a, bb, c), t0, tn) in enumerate(PARTS):
            p2[pi][i].wait_recv()
            if pi == 0:
                pb2[i].wait_recv()
            chunk_send(pi, i + 1, lax.rem(cs[bb] + 4 - d, 4))

    rl = []

    def relay(i):
        for pi, ((a, bb, c), t0, tn) in enumerate(PARTS):
            bi = cs[bb] if i == 0 else lax.rem(cs[bb] + 4 - DELTAS[i - 1], 4)
            h = tn // 2
            for n, (dfrom, dto, lo, cnt) in enumerate(((3, 1, 0, h), (1, 3, h, tn - h))):
                p3[pi][i][n].wait_recv()
                s_ = wslice(cs, (a,), {bb: bi, c: lax.rem(cs[c] + dfrom, 4)}, t0 + lo, cnt)
                rl.append(rc(G.at[s_], G.at[s_], s4.at[pi, i, n], r4.at[pi, i, n], dev(shift(cs, c, dto))))
                if pi == 0:
                    pb3[i][n].wait_recv()
                    b_ = BX.at[lax.rem(y + dfrom, 4), bi, pl.ds(10 * n, 10)]
                    rl.append(rc(b_, b_, sb4.at[i, n], rb4.at[i, n], dev(shift(cs, 0, dto))))

    relay(0)
    routing(cs, routes, gates, modal, cap, st, wt)
    relay(1)
    for c in kvd + kvx_wait:
        c.wait_recv()
    qx.wait_recv()

    scale = HEAD ** (-0.5)
    cxc = []
    for hl in range(2):
        hs = slice(hl * HEAD, (hl + 1) * HEAD)
        first_col = (2 * core + hl) * GROUP
        vt = jnp.transpose(Vb[:, :, hs].reshape(10 * TOK, HEAD).astype(jnp.float32)).astype(jnp.bfloat16)
        for p in range(2):
            kh = Kb[p:p + 9, :, hs].reshape(9 * TOK, HEAD)
            heads = [qb[p, :, (hl * GROUP + g) * HEAD:(hl * GROUP + g + 1) * HEAD] for g in range(GROUP)]
            st_ = lax.dot_general(
                kh, jnp.concatenate(heads, 0), (((1,), (1,)), ((), ())), preferred_element_type=jnp.float32
            ) * scale + jnp.concatenate([bias[p]] * GROUP, 1)
            e = jnp.exp(st_ - jnp.max(st_, 0, keepdims=True))
            tot = jnp.sum(e, 0, keepdims=True)
            o = jnp.dot(
                vt[:, p * TOK:(p + 9) * TOK], e.astype(jnp.bfloat16), preferred_element_type=jnp.float32
            ) / tot
            for g in range(GROUP):
                ctx[first_col + g, :, p * TOK:(p + 1) * TOK] = o[:, g * TOK:(g + 1) * TOK].astype(jnp.bfloat16)
            ready = ctx.at[pl.ds(first_col, GROUP), :, pl.ds(p * TOK, TOK)]
            cxc.append(rc(ready, ready, cxs.at[2 * hl + p], cxr.at[2 * hl + p], sib))
            if hl == 0 and p == 0:
                relay(2)
    for c in cxc:
        c.wait_recv()
    for c in rl + pb3[3] + p3[0][3] + p3[1][3] + p3[2][3]:
        c.wait_recv()

    def project(tile_pair):
        acc = None
        for kp in range(KT // 2):
            rhs = ctx[2 * kp:2 * kp + 2].reshape(2 * HEAD, 2 * TOK)
            part = jnp.dot(tile_pair(2 * kp), rhs, preferred_element_type=jnp.float32)
            acc = part if acc is None else acc + part
        return acc.astype(jnp.bfloat16)

    def put(first, rows, val):
        attp[core, 0, pl.ds(first, rows)] = val[:, :TOK]
        attp[core, 1, pl.ds(first, rows)] = val[:, TOK:]

    def a_rows(yy, carry):
        def pair(t):
            return jnp.concatenate(
                [G[yy, :, :, t + i].reshape(256, 128) for i in range(2)], 1
            )
        put(yy * 256, 256, project(pair))
        return carry

    lax.fori_loop(0, 4, a_rows, 0)
    put(1024, 256, project(
        lambda t: jnp.concatenate([BX[:, :, t + i].reshape(256, 128) for i in range(2)], 1)
    ))
    xc = rc(attp.at[core, 1 - core], attp.at[core, 1 - core], ats, atr, sib)
    xc.wait_recv()
    mine = [attp.at[0, core], attp.at[1, core]]
    for chip in range(64):
        for c in range(2):
            d0 = 20 * (chip * 2 + c)
            attt[d0:d0 + 16] = mine[c][chip * 16:chip * 16 + 16].astype(jnp.float32)
    for yz in range(16):
        for c in range(2):
            blk = mine[c][1024 + yz * 16:1024 + yz * 16 + 16].astype(jnp.float32)
            for xx in range(4):
                d0 = 20 * ((yz * 4 + xx) * 2 + c) + 16
                attt[d0:d0 + 4] = blk[xx * 4:xx * 4 + 4]
    ssq = jnp.zeros((TOK, 1), jnp.float32)
    for t in range(KT):
        ls = slice(t * 128, (t + 1) * 128)
        a_ = jnp.transpose(attt[ls])
        att_out[:, ls] = a_.astype(jnp.bfloat16)
        hd = res[:, ls].astype(jnp.float32) + a_
        ssq = ssq + jnp.sum(hd * hd, -1, keepdims=True)
    inv = lax.rsqrt(ssq / D + 1e-05)
    for t in range(KT):
        ls = slice(t * 128, (t + 1) * 128)
        hd = res[:, ls].astype(jnp.float32) + att_out[:, ls].astype(jnp.float32)
        normed[:, ls] = (hd * inv * gain[ls][None, :]).astype(jnp.bfloat16)


    def offset(i, sign):
        off = order(i)
        full = [4, 4, 4, 2]
        return dev([lax.rem(cs[n] + (off[n] if sign > 0 else full[n] - off[n]), full[n]) for n in range(4)])

    mine = pltpu.make_async_copy(xs.at[0], xr.at[0], dloc)
    for piece in range(2):
        part = slice(piece * NDEV // 2, (piece + 1) * NDEV // 2)
        xs[part] = jnp.dot(
            st[piece * NDEV:(piece + 1) * NDEV], normed[...], preferred_element_type=jnp.float32
        ).astype(jnp.bfloat16).reshape(NDEV // 2, CAP, D)
        if piece == 0:
            mine.start()
        for ch, (first, size) in enumerate(CHUNKS):

            def send(i, c):
                t = offset(i, 1)
                pltpu.make_async_remote_copy(
                    src_ref=xs.at[i], dst_ref=xr.at[i], send_sem=dsem.at[ch], recv_sem=drem.at[ch],
                    device_id=(t,), device_id_type=MESH,
                ).start()
                return c

            low, high = max(1, first, part.start), min(first + size, part.stop)
            if low < high:
                lax.fori_loop(low, high, send, 0)
    mine.wait()

    def whole(src, dst, ch, ss, rs):
        first, size = CHUNKS[ch]
        part = pl.ds(first, size - 1 if first == 0 else size)
        return pltpu.make_async_remote_copy(
            src_ref=src.at[part], dst_ref=dst.at[part], send_sem=ss.at[ch], recv_sem=rs.at[ch],
            device_id=(sib,), device_id_type=MESH,
        )

    for c in weights:
        c.wait()
    nt = (((1,), (1,)), ((), ()))
    home = pltpu.make_async_copy(ys.at[0], ret.at[0], yloc)
    backs = []

    def give_back(ch):
        first, size = CHUNKS[ch]
        count = size * CAP
        flat = pl.ds(first * CAP, count)
        backs[ch].wait_recv()
        ys[first:first + size] = (
            pown[:count].astype(jnp.float32) + precv[flat].astype(jnp.float32)
        ).astype(jnp.bfloat16).reshape(size, CAP, D)

        def give(i, c):
            t = offset(i, -1)
            pltpu.make_async_remote_copy(
                src_ref=ys.at[i], dst_ref=ret.at[i], send_sem=ysem.at[ch], recv_sem=yrem.at[0],
                device_id=(t,), device_id_type=MESH,
            ).start()
            return c

        lax.fori_loop(max(1, first), first + size, give, 0)
        if ch == 0:
            home.start()

    for ch, (first, size) in enumerate(CHUNKS):
        part = pl.ds(first, size)
        count = size * CAP
        flat = pl.ds(first * CAP, count)
        whole(xs, xr, ch, dsem, drem).wait_recv()
        fwd = rc(xr.at[part], xf.at[part], fsem.at[ch], frem.at[ch], sib)
        rows[:count] = xr[part].reshape(count, D)
        if ch > 0:
            give_back(ch - 1)
        fwd.wait_recv()
        rows[count:2 * count] = xf[part].reshape(count, D)
        both = rows[:2 * count]
        gate = lax.dot_general(win[0], both, nt, preferred_element_type=jnp.float32)
        up = lax.dot_general(win[1], both, nt, preferred_element_type=jnp.float32)
        act = jnp.transpose(gate * lax.logistic(gate) * up).astype(jnp.bfloat16)
        psend[flat] = jnp.dot(act[count:], wdn[...], preferred_element_type=jnp.float32).astype(jnp.bfloat16)
        backs.append(rc(psend.at[flat], precv.at[flat], psem.at[ch], prem.at[ch], sib))
        pown[:count] = jnp.dot(act[:count], wdn[...], preferred_element_type=jnp.float32).astype(jnp.bfloat16)
    give_back(len(CHUNKS) - 1)
    home.wait()
    for ch in range(len(CHUNKS)):
        whole(xs, xr, ch, dsem, drem).wait_send()
        whole(ys, ret, ch, ysem, ysem).wait_send()
    every = pl.ds(0, NDEV - 1)
    pltpu.make_async_remote_copy(
        src_ref=ys.at[every], dst_ref=ret.at[every], send_sem=ysem.at[0], recv_sem=yrem.at[0],
        device_id=(sib,), device_id_type=MESH,
    ).wait_recv()
    back_rows = ret[...].reshape(2 * NDEV, D)
    mix = jnp.dot(wt[0], back_rows, preferred_element_type=jnp.float32) + jnp.dot(
        wt[1], back_rows, preferred_element_type=jnp.float32
    )
    mix_out[...] = (mix * (1.0 / 1024.0)).astype(jnp.bfloat16)
    for c in sends:
        c.wait_send()


def out_kernel(a, b, a_out, b_out, sem):
    copies = [pltpu.make_async_copy(a, a_out, sem.at[0]), pltpu.make_async_copy(b, b_out, sem.at[1])]
    for c in copies:
        c.start()
    for c in copies:
        c.wait()


def body(
    residual, queries, keys, values, out_proj, norm_gain, expert_in, expert_down,
    routes, gate_ints, modality, capacity,
):
    any_ = pl.BlockSpec(memory_space=pl.ANY)
    vm = pl.BlockSpec(memory_space=pltpu.VMEM)
    bf = jnp.bfloat16
    cols = expert_in.shape[2]
    outs = pl.pallas_call(
        layer_kernel,
        out_shape=(jax.ShapeDtypeStruct((TOK, D), bf), jax.ShapeDtypeStruct((TOK, D), bf)),
        in_specs=[vm, vm, any_, any_, vm, vm, any_, any_, vm, vm, vm, vm],
        out_specs=(vm, vm),
        scratch_shapes=[
            pltpu.VMEM((4, 4, 4, KT, 16, 128), bf),
            pltpu.VMEM((4, 5, 16, 128), bf),
            pltpu.VMEM((4, 4, KT, 16, 128), bf),
            pltpu.VMEM((2, TOK, KV_HEADS * HEAD // 2), bf),
            pltpu.VMEM((2, TOK, KV_HEADS * HEAD // 2), bf),
            pltpu.VMEM((10, TOK, KV_HEADS * HEAD // 2), bf),
            pltpu.VMEM((10, TOK, KV_HEADS * HEAD // 2), bf),
            pltpu.VMEM((2, TOK, D // 2), bf),
            pltpu.VMEM((2, 9 * TOK, TOK), jnp.float32),
            pltpu.VMEM((KT, HEAD, 2 * TOK), bf),
            pltpu.VMEM((2, 2, 1280, TOK), bf),
            pltpu.VMEM((D, TOK), jnp.float32),
            pltpu.VMEM((TOK, D), bf),
            pltpu.VMEM((2 * NDEV, TOK), bf),
            pltpu.VMEM((2, TOK, 2 * NDEV), bf),
            pltpu.VMEM((2, cols, D), bf),
            pltpu.VMEM((cols, D), bf),
            pltpu.VMEM((NDEV, CAP, D), bf),
            pltpu.VMEM((NDEV, CAP, D), bf),
            pltpu.VMEM((NDEV, CAP, D), bf),
            pltpu.VMEM((2 * TOK, D), bf),
            pltpu.VMEM((TOK, D), bf),
            pltpu.VMEM((2 * TOK, D), bf),
            pltpu.VMEM((2 * TOK, D), bf),
            pltpu.VMEM((NDEV, CAP, D), bf),
            pltpu.VMEM((NDEV, CAP, D), bf),
            DMA((3, 3)), DMA((3, 3)), DMA((3, 3)), DMA((3, 3)),
            DMA((3, 4, 3)), DMA((3, 4, 3)), DMA((3, 4, 2)), DMA((3, 4, 2)),
            DMA((3,)), DMA((3,)), DMA((3,)), DMA((3,)),
            DMA((4, 3)), DMA((4, 3)), DMA((4, 2)), DMA((4, 2)),
            DMA((2, 2)), DMA((2, 2)), DMA((2, 3, 2)), DMA((2, 3, 2)), DMA((2,)), DMA((2,)),
            DMA((5,)), DMA((5,)), DMA, DMA, DMA((8,)),
            DMA((4,)), DMA((4,)), DMA, DMA((4,)), DMA((4,)), DMA((4,)), DMA((4,)), DMA((4,)), DMA((1,)), DMA,
        ],
        compiler_params=pltpu.CompilerParams(
            has_side_effects=True, collective_id=0, vmem_limit_bytes=60 * 2**20
        ),
    )(
        out_proj.T, queries, keys, values, residual, norm_gain, expert_in.transpose(1, 2, 0), expert_down,
        routes.T, gate_ints.T, modality, capacity.T,
    )
    shape = jax.ShapeDtypeStruct((TOK, D), bf)
    return pl.pallas_call(
        out_kernel, out_shape=(shape, shape), in_specs=[vm, vm], out_specs=(any_, any_), scratch_shapes=[DMA((2,))],
        compiler_params=pltpu.CompilerParams(vmem_limit_bytes=4 * 2**20),
    )(*outs)


def solution(mesh):
    placed = (
        P("seq", None), P("seq", None), P("seq", None), P("seq", None), P(None, "seq"), P(),
        P(None, None, "seq"), P("seq", None), P("seq", None), P("seq", None), P("seq"), P(),
    )
    return jax.shard_map(
        body, mesh=mesh, in_specs=placed, out_specs=(P("seq", None), P("seq", None)), check_vma=False
    )
```

```python
import functools

import jax
import jax.numpy as jnp
from jax import lax
from jax.experimental import pallas as pl
from jax.experimental.pallas import tpu as pltpu
from jax.sharding import PartitionSpec as P

HEADS = 20
KV_HEADS = 4
HEAD = 128
GROUP = HEADS // KV_HEADS
WINDOW = 1024
EXPERTS = 64
CAP = 2
D = 2560
TOK = 128
NDEV = 128
MESH = pl.DeviceIdType.MESH
DMA = pltpu.SemaphoreType.DMA
DELTAS = (1, 3, 2)
PARTS = (((2, 1, 0), 0, 4), ((1, 0, 2), 4, 8), ((2, 0, 1), 12, 8))
CHUNKS = ((0, 64), (64, 64))
KT = D // 128


def coords(me):
    return [me // 32, (me // 8) % 4, (me // 2) % 4, me % 2]


def dev(cs):
    return ((cs[0] * 4 + cs[1]) * 4 + cs[2]) * 2 + cs[3]


def shift(cs, dim, d):
    cs = list(cs)
    cs[dim] = lax.rem(cs[dim] + d, 4)
    return cs


def wslice(cs, alld, fixed, t0, tn):
    idx = [slice(None) if d in alld else cs[d] for d in range(3)]
    for d, v in fixed.items():
        idx[d] = v
    return tuple(idx) + (pl.ds(t0, tn),)


def order(i):
    s = (i * 59) % NDEV
    return [s // 32, (s // 8) % 4, (s // 2) % 4, s % 2]


def routing(cs, routes, gates, modal, cap, st, wt):
    rows = 2 * NDEV
    rho = lax.broadcasted_iota(jnp.int32, (rows, TOK), 0)
    turn = jnp.bitwise_and(rho, 1)

    def device(at):
        off = jnp.bitwise_and(jnp.right_shift(at, 1) * 59, NDEV - 1)
        y, z, x, core = cs
        ny = jnp.bitwise_and(y + jnp.right_shift(off, 5), 3)
        nz = jnp.bitwise_and(z + jnp.bitwise_and(jnp.right_shift(off, 3), 3), 3)
        nx = jnp.bitwise_and(x + jnp.bitwise_and(jnp.right_shift(off, 1), 3), 3)
        return ny * 32 + nz * 8 + nx * 2 + jnp.bitwise_and(core + off, 1)

    key = device(rho)
    mod = modal[...][None, :]
    is0 = key == routes[0:1] * 2 + mod
    is1 = key == routes[1:2] * 2 + mod
    hit = jnp.where(is0 | is1, 1.0, 0.0)
    before = lax.broadcasted_iota(jnp.int32, (TOK, TOK), 0) < lax.broadcasted_iota(jnp.int32, (TOK, TOK), 1)
    rank = jnp.dot(
        hit.astype(jnp.bfloat16), jnp.where(before, 1.0, 0.0).astype(jnp.bfloat16),
        preferred_element_type=jnp.float32,
    )
    key_e = device(lax.broadcasted_iota(jnp.int32, (rows, EXPERTS), 0))
    at_e = lax.broadcasted_iota(jnp.int32, (rows, EXPERTS), 1) == jnp.right_shift(key_e, 1)
    cap_e = jnp.where(jnp.bitwise_and(key_e, 1) == 0, cap[0:1], cap[1:2]).astype(jnp.float32)
    limit = jnp.sum(jnp.where(at_e, cap_e, 0.0), -1, keepdims=True)
    turn_f = turn.astype(jnp.float32)
    kept = jnp.where((rank == turn_f) & (turn_f < limit), hit, 0.0)
    st[...] = kept.astype(jnp.bfloat16)
    g = jnp.where(is0, gates[0:1], gates[1:2])
    high = jnp.bitwise_and(g, 1016)
    wt[0] = jnp.transpose(high.astype(jnp.float32) * kept).astype(jnp.bfloat16)
    wt[1] = jnp.transpose((g - high).astype(jnp.float32) * kept).astype(jnp.bfloat16)


def layer_kernel(
    w, q, k, v, res, gain, w_in, w_down, routes, gates, modal, cap, att_out, mix_out, att_v, att_sem,
    G, B1, BX, Ko, Vo, Kb, Vb, qb, bias, ctx, attp, attt, normed, st, wt, win, wdn,
    xs, xr, xf, rows, pown, psend, precv, ys, ret,
    s1, r1, s2, r2, s3, r3, s4, r4, sb1, rb1, sb2, rb2, sb3, rb3, sb4, rb4,
    kzs, kzr, kxs, kxr, kds, kdr, cxs, cxr, ats, atr, lsem,
    dsem, drem, dloc, fsem, frem, psem, prem, ysem, yrem, yloc,
):
    me = lax.axis_index("seq")
    cs = coords(me)
    y, z, x, core = cs
    bar = pltpu.get_barrier_semaphore()
    sib = dev([y, z, x, 1 - core])

    def signal(i, c):
        pl.semaphore_signal(bar, inc=1, device_id=(lax.rem(me + i, NDEV),), device_id_type=MESH)
        return c

    lax.fori_loop(1, NDEV, signal, 0)
    half_w = KV_HEADS * HEAD // 2
    own = []
    for n, (src, own_, buf) in enumerate(((k, Ko, Kb), (v, Vo, Vb))):
        for hf in range(2):
            own.append(pltpu.make_async_copy(src.at[:, pl.ds(hf * half_w, half_w)], own_.at[hf], lsem.at[3 * n + hf]))
        own.append(pltpu.make_async_copy(
            src.at[:, pl.ds(pl.multiple_of(core * half_w, half_w), half_w)], buf.at[8 + core], lsem.at[3 * n + 2]
        ))
    for c in own:
        c.start()
    weights = [
        pltpu.make_async_copy(w_in, win, lsem.at[6]),
        pltpu.make_async_copy(w_down, wdn, lsem.at[7]),
    ]
    for c in weights:
        c.start()
    for t in range(KT):
        G[y, z, x, t] = w[0:16, t * 128:(t + 1) * 128]
    tail = w[16:20].astype(jnp.float32)
    for i in range(5):
        B1[x, i] = jnp.concatenate(
            [tail[:, n * 640 + i * 128:n * 640 + i * 128 + 128] for n in range(4)], 0
        ).astype(jnp.bfloat16)
    key_at = lax.broadcasted_iota(jnp.int32, (TOK, TOK), 0)
    query_at = lax.broadcasted_iota(jnp.int32, (TOK, TOK), 1)
    for p in range(2):
        for j in range(9):
            ok = me - core - 8 + j + p >= 0
            if j == 0:
                m = (key_at > query_at) & ok
            elif j == 8:
                m = key_at <= query_at
            else:
                m = (key_at >= 0) & ok
            bias[p, j * TOK:(j + 1) * TOK] = jnp.where(m, 0.0, -jnp.inf)
    mine_q = pl.ds(pl.multiple_of(core * (D // 2), 128), D // 2)
    qb[core] = q[:, mine_q]
    for c in own:
        c.wait()
    pl.semaphore_wait(bar, NDEV - 1)
    sends = []

    def rc(src, dst, ss, rs, dv):
        c = pltpu.make_async_remote_copy(
            src_ref=src, dst_ref=dst, send_sem=ss, recv_sem=rs, device_id=(dv,), device_id_type=MESH
        )
        c.start()
        sends.append(c)
        return c

    p1 = []
    for pi, ((a, bb, c), t0, tn) in enumerate(PARTS):
        sl = wslice(cs, (), {}, t0, tn)
        p1.append(
            [rc(G.at[sl], G.at[sl], s1.at[pi, i], r1.at[pi, i], dev(shift(cs, a, d))) for i, d in enumerate(DELTAS)]
        )
    pb1 = [rc(B1.at[x], B1.at[x], sb1.at[i], rb1.at[i], dev(shift(cs, 2, d))) for i, d in enumerate(DELTAS)]

    def twin(cs_, c_):
        return dev(cs_[:3] + [c_])

    kvz, kvx, kvx_wait = [], [], []
    up = lax.rem(me - core + 8, NDEV)
    for n, (own_, buf) in enumerate(((Ko, Kb), (Vo, Vb))):
        for hf in range(2):
            kvz.append(rc(own_.at[hf], buf.at[core], kzs.at[n, hf], kzr.at[n, core], up + hf))
    qx = rc(q.at[:, pl.ds(pl.multiple_of((1 - core) * (D // 2), 128), D // 2)], qb.at[core], cxs.at[4], cxr.at[4], sib)
    kvd = [
        rc(own_.at[1 - core], buf.at[8 + core], kds.at[n], kdr.at[n], sib)
        for n, (own_, buf) in enumerate(((Ko, Kb), (Vo, Vb)))
    ]
    for dlt in (1, 3, 2):
        tgt = shift(cs, 2, dlt)
        for n, (own_, buf) in enumerate(((Ko, Kb), (Vo, Vb))):
            for hf in range(2):
                slot = (4 - dlt) * 2
                fresh = pltpu.make_async_remote_copy(
                    src_ref=own_.at[hf], dst_ref=buf.at[slot + core], send_sem=kxs.at[n, dlt - 1, hf],
                    recv_sem=kxr.at[n, dlt - 1, core], device_id=(twin(tgt, hf),), device_id_type=MESH,
                )
                older = pltpu.make_async_remote_copy(
                    src_ref=buf.at[hf], dst_ref=buf.at[slot + hf], send_sem=kxs.at[n, dlt - 1, hf],
                    recv_sem=kxr.at[n, dlt - 1, hf], device_id=(twin(tgt, core),), device_id_type=MESH,
                )
                kvx.append((n, dlt, fresh, older))
                kvx_wait.append(older)

    for n, dlt, fresh, older in kvx:
        sends.append(older)

        @pl.when(x + dlt < 4)
        def _():
            fresh.start()

    p3 = [[None] * 4 for _ in PARTS]
    pb3 = [None] * 4

    def chunk_send(pi, i, bi):
        (a, bb, c), t0, tn = PARTS[pi]
        sl = wslice(cs, (a,), {bb: bi}, t0, tn)
        p3[pi][i] = [
            rc(G.at[sl], G.at[sl], s3.at[pi, i, n], r3.at[pi, i, n], dev(shift(cs, c, d)))
            for n, d in enumerate(DELTAS[:3 if i == 3 else 2])
        ]
        if pi == 0:
            pb3[i] = [
                rc(BX.at[y, bi], BX.at[y, bi], sb3.at[i, n], rb3.at[i, n], dev(shift(cs, 0, d)))
                for n, d in enumerate(DELTAS[:3 if i == 3 else 2])
            ]

    p2 = [None] * 3
    pb2 = []
    for pi in (0, 2, 1):
        (a, bb, c), t0, tn = PARTS[pi]
        for n in range(3):
            p1[pi][n].wait_recv()
        if pi == 0:
            for n in range(3):
                pb1[n].wait_recv()
            src = [[B1[xx, i].astype(jnp.float32) for i in range(5)] for xx in range(4)]
            for kq in range(4):
                for i in range(5):
                    BX[y, z, kq * 5 + i] = jnp.concatenate(
                        [src[xx][i][kq * 4:kq * 4 + 4] for xx in range(4)], 0
                    ).astype(jnp.bfloat16)
        sl = wslice(cs, (a,), {}, t0, tn)
        p2[pi] = [
            rc(G.at[sl], G.at[sl], s2.at[pi, i], r2.at[pi, i], dev(shift(cs, bb, d))) for i, d in enumerate(DELTAS)
        ]
        if pi == 0:
            pb2 = [
                rc(BX.at[y, z], BX.at[y, z], sb2.at[i], rb2.at[i], dev(shift(cs, 1, d)))
                for i, d in enumerate(DELTAS)
            ]
        chunk_send(pi, 0, cs[bb])

    for n, buf in enumerate((Kb, Vb)):
        for hf in range(2):
            pltpu.make_async_remote_copy(
                src_ref=buf.at[hf], dst_ref=buf.at[hf], send_sem=kzs.at[n, hf], recv_sem=kzr.at[n, hf],
                device_id=(up,), device_id_type=MESH,
            ).wait_recv()
        for n_, dlt, fresh, older in kvx:
            if n_ == n:

                @pl.when(x + dlt >= 4)
                def _():
                    older.start()

    for i, d in enumerate(DELTAS):
        for pi, ((a, bb, c), t0, tn) in enumerate(PARTS):
            p2[pi][i].wait_recv()
            if pi == 0:
                pb2[i].wait_recv()
            chunk_send(pi, i + 1, lax.rem(cs[bb] + 4 - d, 4))

    rl = []

    def relay(i):
        for pi, ((a, bb, c), t0, tn) in enumerate(PARTS):
            bi = cs[bb] if i == 0 else lax.rem(cs[bb] + 4 - DELTAS[i - 1], 4)
            h = tn // 2
            for n, (dfrom, dto, lo, cnt) in enumerate(((3, 1, 0, h), (1, 3, h, tn - h))):
                p3[pi][i][n].wait_recv()
                s_ = wslice(cs, (a,), {bb: bi, c: lax.rem(cs[c] + dfrom, 4)}, t0 + lo, cnt)
                rl.append(rc(G.at[s_], G.at[s_], s4.at[pi, i, n], r4.at[pi, i, n], dev(shift(cs, c, dto))))
                if pi == 0:
                    pb3[i][n].wait_recv()
                    b_ = BX.at[lax.rem(y + dfrom, 4), bi, pl.ds(10 * n, 10)]
                    rl.append(rc(b_, b_, sb4.at[i, n], rb4.at[i, n], dev(shift(cs, 0, dto))))

    relay(0)
    routing(cs, routes, gates, modal, cap, st, wt)
    relay(1)
    for c in kvd + kvx_wait:
        c.wait_recv()
    qx.wait_recv()

    scale = HEAD ** (-0.5)
    cxc = []
    for hl in range(2):
        hs = slice(hl * HEAD, (hl + 1) * HEAD)
        first_col = (2 * core + hl) * GROUP
        vt = jnp.transpose(Vb[:, :, hs].reshape(10 * TOK, HEAD).astype(jnp.float32)).astype(jnp.bfloat16)
        for p in range(2):
            kh = Kb[p:p + 9, :, hs].reshape(9 * TOK, HEAD)
            heads = [qb[p, :, (hl * GROUP + g) * HEAD:(hl * GROUP + g + 1) * HEAD] for g in range(GROUP)]
            st_ = lax.dot_general(
                kh, jnp.concatenate(heads, 0), (((1,), (1,)), ((), ())), preferred_element_type=jnp.float32
            ) * scale + jnp.concatenate([bias[p]] * GROUP, 1)
            e = jnp.exp(st_ - jnp.max(st_, 0, keepdims=True))
            tot = jnp.sum(e, 0, keepdims=True)
            o = jnp.dot(
                vt[:, p * TOK:(p + 9) * TOK], e.astype(jnp.bfloat16), preferred_element_type=jnp.float32
            ) / tot
            for g in range(GROUP):
                ctx[first_col + g, :, p * TOK:(p + 1) * TOK] = o[:, g * TOK:(g + 1) * TOK].astype(jnp.bfloat16)
            ready = ctx.at[pl.ds(first_col, GROUP), :, pl.ds(p * TOK, TOK)]
            cxc.append(rc(ready, ready, cxs.at[2 * hl + p], cxr.at[2 * hl + p], sib))
            if hl == 0 and p == 1:
                relay(2)
    for c in cxc:
        c.wait_recv()
    for c in rl + pb3[3] + p3[0][3] + p3[1][3] + p3[2][3]:
        c.wait_recv()

    def project(tile_pair):
        acc = None
        for kp in range(KT // 2):
            rhs = ctx[2 * kp:2 * kp + 2].reshape(2 * HEAD, 2 * TOK)
            part = jnp.dot(tile_pair(2 * kp), rhs, preferred_element_type=jnp.float32)
            acc = part if acc is None else acc + part
        return acc.astype(jnp.bfloat16)

    def put(first, rows, val):
        attp[core, 0, pl.ds(first, rows)] = val[:, :TOK]
        attp[core, 1, pl.ds(first, rows)] = val[:, TOK:]

    def a_rows(yy, carry):
        def pair(t):
            return jnp.concatenate(
                [G[yy, :, :, t + i].reshape(256, 128) for i in range(2)], 1
            )
        put(yy * 256, 256, project(pair))
        return carry

    lax.fori_loop(0, 4, a_rows, 0)
    put(1024, 256, project(
        lambda t: jnp.concatenate([BX[:, :, t + i].reshape(256, 128) for i in range(2)], 1)
    ))
    xc = rc(attp.at[core, 1 - core], attp.at[core, 1 - core], ats, atr, sib)
    xc.wait_recv()
    mine = [attp.at[0, core], attp.at[1, core]]
    for chip in range(64):
        for c in range(2):
            d0 = 20 * (chip * 2 + c)
            attt[d0:d0 + 16] = mine[c][chip * 16:chip * 16 + 16].astype(jnp.float32)
    for yz in range(16):
        for c in range(2):
            blk = mine[c][1024 + yz * 16:1024 + yz * 16 + 16].astype(jnp.float32)
            for xx in range(4):
                d0 = 20 * ((yz * 4 + xx) * 2 + c) + 16
                attt[d0:d0 + 4] = blk[xx * 4:xx * 4 + 4]
    ssq = jnp.zeros((TOK, 1), jnp.float32)
    for t in range(KT):
        ls = slice(t * 128, (t + 1) * 128)
        a_ = jnp.transpose(attt[ls])
        att_v[:, ls] = a_.astype(jnp.bfloat16)
        hd = res[:, ls].astype(jnp.float32) + a_
        ssq = ssq + jnp.sum(hd * hd, -1, keepdims=True)
    inv = lax.rsqrt(ssq / D + 1e-05)
    for t in range(KT):
        ls = slice(t * 128, (t + 1) * 128)
        hd = res[:, ls].astype(jnp.float32) + att_v[:, ls].astype(jnp.float32)
        normed[:, ls] = (hd * inv * gain[ls][None, :]).astype(jnp.bfloat16)

    early = pltpu.make_async_copy(att_v, att_out, att_sem)

    def offset(i, sign):
        off = order(i)
        full = [4, 4, 4, 2]
        return dev([lax.rem(cs[n] + (off[n] if sign > 0 else full[n] - off[n]), full[n]) for n in range(4)])

    mine = pltpu.make_async_copy(xs.at[0], xr.at[0], dloc)
    for piece in range(2):
        part = slice(piece * NDEV // 2, (piece + 1) * NDEV // 2)
        xs[part] = jnp.dot(
            st[piece * NDEV:(piece + 1) * NDEV], normed[...], preferred_element_type=jnp.float32
        ).astype(jnp.bfloat16).reshape(NDEV // 2, CAP, D)
        if piece == 0:
            mine.start()
        for ch, (first, size) in enumerate(CHUNKS):

            def send(i, c):
                t = offset(i, 1)
                pltpu.make_async_remote_copy(
                    src_ref=xs.at[i], dst_ref=xr.at[i], send_sem=dsem.at[ch], recv_sem=drem.at[ch],
                    device_id=(t,), device_id_type=MESH,
                ).start()
                return c

            low, high = max(1, first, part.start), min(first + size, part.stop)
            if low < high:
                lax.fori_loop(low, high, send, 0)
    mine.wait()
    early.start()

    def whole(src, dst, ch, ss, rs):
        first, size = CHUNKS[ch]
        part = pl.ds(first, size - 1 if first == 0 else size)
        return pltpu.make_async_remote_copy(
            src_ref=src.at[part], dst_ref=dst.at[part], send_sem=ss.at[ch], recv_sem=rs.at[ch],
            device_id=(sib,), device_id_type=MESH,
        )

    for c in weights:
        c.wait()
    nt = (((1,), (1,)), ((), ()))
    home = pltpu.make_async_copy(ys.at[0], ret.at[0], yloc)
    backs = []

    def give_back(ch):
        first, size = CHUNKS[ch]
        count = size * CAP
        flat = pl.ds(first * CAP, count)
        backs[ch].wait_recv()
        ys[first:first + size] = (
            pown[:count].astype(jnp.float32) + precv[flat].astype(jnp.float32)
        ).astype(jnp.bfloat16).reshape(size, CAP, D)

        def give(i, c):
            t = offset(i, -1)
            pltpu.make_async_remote_copy(
                src_ref=ys.at[i], dst_ref=ret.at[i], send_sem=ysem.at[ch], recv_sem=yrem.at[0],
                device_id=(t,), device_id_type=MESH,
            ).start()
            return c

        lax.fori_loop(max(1, first), first + size, give, 0)
        if ch == 0:
            home.start()

    for ch, (first, size) in enumerate(CHUNKS):
        part = pl.ds(first, size)
        count = size * CAP
        flat = pl.ds(first * CAP, count)
        whole(xs, xr, ch, dsem, drem).wait_recv()
        fwd = rc(xr.at[part], xf.at[part], fsem.at[ch], frem.at[ch], sib)
        rows[:count] = xr[part].reshape(count, D)
        if ch > 0:
            give_back(ch - 1)
        fwd.wait_recv()
        rows[count:2 * count] = xf[part].reshape(count, D)
        both = rows[:2 * count]
        gate = lax.dot_general(win[0], both, nt, preferred_element_type=jnp.float32)
        up = lax.dot_general(win[1], both, nt, preferred_element_type=jnp.float32)
        act = jnp.transpose(gate * lax.logistic(gate) * up).astype(jnp.bfloat16)
        psend[flat] = jnp.dot(act[count:], wdn[...], preferred_element_type=jnp.float32).astype(jnp.bfloat16)
        backs.append(rc(psend.at[flat], precv.at[flat], psem.at[ch], prem.at[ch], sib))
        pown[:count] = jnp.dot(act[:count], wdn[...], preferred_element_type=jnp.float32).astype(jnp.bfloat16)
    give_back(len(CHUNKS) - 1)
    home.wait()
    for ch in range(len(CHUNKS)):
        whole(xs, xr, ch, dsem, drem).wait_send()
        whole(ys, ret, ch, ysem, ysem).wait_send()
    every = pl.ds(0, NDEV - 1)
    pltpu.make_async_remote_copy(
        src_ref=ys.at[every], dst_ref=ret.at[every], send_sem=ysem.at[0], recv_sem=yrem.at[0],
        device_id=(sib,), device_id_type=MESH,
    ).wait_recv()
    back_rows = ret[...].reshape(2 * NDEV, D)
    mix = jnp.dot(wt[0], back_rows, preferred_element_type=jnp.float32) + jnp.dot(
        wt[1], back_rows, preferred_element_type=jnp.float32
    )
    mix_out[...] = (mix * (1.0 / 1024.0)).astype(jnp.bfloat16)
    early.wait()
    for c in sends:
        c.wait_send()


def out_kernel(a, b, a_out, b_out, a_buf, b_buf, sem_in, sem_out):
    loads, stores = [], []
    for n, (src, buf, dst) in enumerate(((a, a_buf, a_out), (b, b_buf, b_out))):
        for h in range(2):
            part = pl.ds(h * TOK // 2, TOK // 2)
            loads.append(pltpu.make_async_copy(src.at[part], buf.at[part], sem_in.at[n, h]))
            stores.append(pltpu.make_async_copy(buf.at[part], dst.at[part], sem_out.at[n, h]))
    for c in loads:
        c.start()
    for c, d in zip(loads, stores):
        c.wait()
        d.start()
    for d in stores:
        d.wait()


def body(
    residual, queries, keys, values, out_proj, norm_gain, expert_in, expert_down,
    routes, gate_ints, modality, capacity,
):
    any_ = pl.BlockSpec(memory_space=pl.ANY)
    vm = pl.BlockSpec(memory_space=pltpu.VMEM)
    bf = jnp.bfloat16
    cols = expert_in.shape[2]
    outs = pl.pallas_call(
        layer_kernel,
        out_shape=(jax.ShapeDtypeStruct((TOK, D), bf), jax.ShapeDtypeStruct((TOK, D), bf)),
        in_specs=[vm, vm, any_, any_, vm, vm, any_, any_, vm, vm, vm, vm],
        out_specs=(any_, vm),
        scratch_shapes=[
            pltpu.VMEM((TOK, D), bf),
            DMA,
            pltpu.VMEM((4, 4, 4, KT, 16, 128), bf),
            pltpu.VMEM((4, 5, 16, 128), bf),
            pltpu.VMEM((4, 4, KT, 16, 128), bf),
            pltpu.VMEM((2, TOK, KV_HEADS * HEAD // 2), bf),
            pltpu.VMEM((2, TOK, KV_HEADS * HEAD // 2), bf),
            pltpu.VMEM((10, TOK, KV_HEADS * HEAD // 2), bf),
            pltpu.VMEM((10, TOK, KV_HEADS * HEAD // 2), bf),
            pltpu.VMEM((2, TOK, D // 2), bf),
            pltpu.VMEM((2, 9 * TOK, TOK), jnp.float32),
            pltpu.VMEM((KT, HEAD, 2 * TOK), bf),
            pltpu.VMEM((2, 2, 1280, TOK), bf),
            pltpu.VMEM((D, TOK), jnp.float32),
            pltpu.VMEM((TOK, D), bf),
            pltpu.VMEM((2 * NDEV, TOK), bf),
            pltpu.VMEM((2, TOK, 2 * NDEV), bf),
            pltpu.VMEM((2, cols, D), bf),
            pltpu.VMEM((cols, D), bf),
            pltpu.VMEM((NDEV, CAP, D), bf),
            pltpu.VMEM((NDEV, CAP, D), bf),
            pltpu.VMEM((NDEV, CAP, D), bf),
            pltpu.VMEM((2 * TOK, D), bf),
            pltpu.VMEM((TOK, D), bf),
            pltpu.VMEM((2 * TOK, D), bf),
            pltpu.VMEM((2 * TOK, D), bf),
            pltpu.VMEM((NDEV, CAP, D), bf),
            pltpu.VMEM((NDEV, CAP, D), bf),
            DMA((3, 3)), DMA((3, 3)), DMA((3, 3)), DMA((3, 3)),
            DMA((3, 4, 3)), DMA((3, 4, 3)), DMA((3, 4, 2)), DMA((3, 4, 2)),
            DMA((3,)), DMA((3,)), DMA((3,)), DMA((3,)),
            DMA((4, 3)), DMA((4, 3)), DMA((4, 2)), DMA((4, 2)),
            DMA((2, 2)), DMA((2, 2)), DMA((2, 3, 2)), DMA((2, 3, 2)), DMA((2,)), DMA((2,)),
            DMA((5,)), DMA((5,)), DMA, DMA, DMA((8,)),
            DMA((4,)), DMA((4,)), DMA, DMA((4,)), DMA((4,)), DMA((4,)), DMA((4,)), DMA((4,)), DMA((1,)), DMA,
        ],
        compiler_params=pltpu.CompilerParams(
            has_side_effects=True, collective_id=0, vmem_limit_bytes=60 * 2**20
        ),
    )(
        out_proj.T, queries, keys, values, residual, norm_gain, expert_in.transpose(1, 2, 0), expert_down,
        routes.T, gate_ints.T, modality, capacity.T,
    )
    shape = jax.ShapeDtypeStruct((TOK, D), bf)
    return pl.pallas_call(
        out_kernel,
        out_shape=(shape, shape),
        in_specs=[any_, any_],
        out_specs=(any_, any_),
        scratch_shapes=[pltpu.VMEM((TOK, D), bf), pltpu.VMEM((TOK, D), bf), DMA((2, 2)), DMA((2, 2))],
        compiler_params=pltpu.CompilerParams(vmem_limit_bytes=60 * 2**20),
    )(*outs)


def solution(mesh):
    placed = (
        P("seq", None), P("seq", None), P("seq", None), P("seq", None), P(None, "seq"), P(),
        P(None, None, "seq"), P("seq", None), P("seq", None), P("seq", None), P("seq"), P(),
    )
    return jax.shard_map(
        body, mesh=mesh, in_specs=placed, out_specs=(P("seq", None), P("seq", None)), check_vma=False
    )
```
